32 devices in a mesh: group: 8 (over y, x, core), head: 4 (over z).
Axes of the slice: x: 2, y: 2, z: 4, core: 2. Of those that a mesh axis runs over, the one named last changes fastest.
Arguments:
- hidden_in: bfloat16 [128, 2560], P('group'), may hold values from -6 to 6
- ssm_state: float32 [128, 80, 64, 128], P('group', 'head'), may hold values from -6 to 6
- conv_x_state: bfloat16 [128, 3, 5120], P('group', None, 'head'), may hold values from -6 to 6
- conv_bc_state: bfloat16 [128, 3, 256], P('group'), may hold values from -6 to 6
- token_ids: int32 [128], P('group'), may hold values from 0 to 25599
- ref_logits: bfloat16 [128, 25600], P('group', 'head'), may hold values from -15 to 350
- in_z: bfloat16 [2560, 5120], P('group', 'head'), may hold values from -0.125 to 0.125
- in_x: bfloat16 [2560, 5120], P('group', 'head'), may hold values from -0.125 to 0.125
- in_bc: bfloat16 [2560, 256], P('group'), may hold values from -0.125 to 0.125
- in_dt: bfloat16 [2560, 80], P('group', 'head'), may hold values from -0.125 to 0.125
- out_t: bfloat16 [2560, 5120], P('group', 'head'), may hold values from -0.078125 to 0.078125
- lm_head: bfloat16 [25600, 2560], P('head', 'group'), may hold values from -6 to 6
- conv_wx: float32 [4, 5120], P(None, 'head'), may hold values from -3 to 3
- conv_bx: float32 [5120], P('head'), may hold values from -1.5 to 1.5
- conv_wbc: float32 [4, 256], replicated, may hold values from -3 to 3
- conv_bbc: float32 [256], replicated, may hold values from -1.5 to 1.5
- dt_bias: float32 [80], P('head'), may hold values from -4 to -1
- a_log: float32 [80], P('head'), may hold values from 0 to 2.77
- skip_gain: float32 [80], P('head'), may hold values from 0.5 to 1.5
- norm_in: float32 [2560], replicated, may hold values from 0.5 to 1.5
- norm_gain: float32 [5120], P('head'), may hold values from 0.5 to 1.5
- final_gain: float32 [2560], replicated, may hold values from 0.5 to 1.5
Outputs:
- new_state: float32 [128, 80, 64, 128], P('group', 'head')
- divergence: float32 [128], P('group')
- token_logprob: float32 [128], P('group')
- roll_z: bfloat16 [2560, 5120], P(None, 'head')
- roll_x: bfloat16 [2560, 5120], P(None, 'head')
- roll_bc: bfloat16 [2560, 256], replicated
- roll_dt: bfloat16 [2560, 80], P(None, 'head')
- roll_out: bfloat16 [2560, 5120], P(None, 'head')
The draws below stay inside these ranges and needn't reach their ends.
All inputs are finite; a program needn't handle non-finite values.
Results may differ from the reference program's by a relative error of at most 0.0102.
Values may be sent and summed in bfloat16 or wider, within the bound.
A program may use at most 128 MiB of HBM per device.

```python
import math
import jax
import jax.numpy as jnp
from jax import lax

D = 2560
H = 80
P_SIZE = 64
N = 128
KCONV = 4
V = 25600
SEQS = 16
DI = 5120
SEQ_ALL = 128
N_GROUP = 8


def draw_lm_head(key, part):
    subkeys = jax.random.split(key, 1)
    values = jax.random.normal(subkeys[0], (V, D), jnp.float32) * (3.0 / math.sqrt(D))
    return jnp.clip(values, -6.0, 6.0).astype(jnp.bfloat16)


def draw_ref_logits(key, part):
    subkeys = jax.random.split(key, 1)
    total_rows = SEQS * N_GROUP
    values = jnp.clip(jax.random.normal(subkeys[0], (total_rows, V), jnp.float32) * 3.0, -15.0, 15.0)
    return values.astype(jnp.bfloat16)


def place_ends(drawn, key, least, largest):
    place = [jax.random.randint(jax.random.fold_in(key, axis), (), 0, length) for axis, length in enumerate(drawn.shape)]
    longest = drawn.shape.index(max(drawn.shape))
    neighbour = place[:longest] + [(place[longest] + 1) % drawn.shape[longest]] + place[longest + 1:]
    return drawn.at[tuple(place)].set(least).at[tuple(neighbour)].set(largest)


def level_of(key, shape, pieces, smallest, top_value):
    level = 1.0
    for axis_at, shards_of in pieces:
        steps = jax.random.uniform(jax.random.fold_in(jax.random.fold_in(key, 6), axis_at), (shards_of,), jnp.float32, smallest / len(pieces), top_value / len(pieces))
        level = level * jnp.repeat(jnp.exp(steps), shape[axis_at] // shards_of).reshape((-1,) + (1,) * (len(shape) - 1 - axis_at))
    return level


def scatter_about(key, extent, scale, limit, pieces=(), held_as=jnp.bfloat16):
    entries = scale * jax.random.normal(key, extent, jnp.float32)
    if pieces:
        entries = entries * level_of(key, extent, pieces, -0.22, 0.18)
    return jnp.clip(entries, -limit, limit).astype(held_as)


def setup_inputs(seed: int = 0) -> dict:
    arg_keys = jax.random.split(jax.random.key(seed), 23)
    hidden_in = scatter_about(arg_keys[0], (SEQ_ALL, D), 1.0, 6.0, ((0, 8),))
    ssm_state = scatter_about(arg_keys[1], (SEQ_ALL, H, P_SIZE, N), 1.0, 6.0, ((0, 8), (1, 4)), jnp.float32)
    conv_x_state = scatter_about(arg_keys[2], (SEQ_ALL, KCONV - 1, DI), 1.0, 6.0, ((0, 8), (2, 4)))
    conv_bc_state = scatter_about(arg_keys[3], (SEQ_ALL, KCONV - 1, 2 * N), 1.0, 6.0, ((0, 8),))
    token_ids = place_ends(jax.random.randint(arg_keys[4], (SEQ_ALL,), 0, V), jax.random.fold_in(arg_keys[4], 1), 0, V - 1).astype(jnp.int32)
    ref_logits = draw_ref_logits(jax.random.fold_in(arg_keys[22], 71), 0)
    in_z = scatter_about(arg_keys[6], (D, DI), D ** -0.5, 0.125, ((0, 8), (1, 4)))
    in_x = scatter_about(arg_keys[7], (D, DI), D ** -0.5, 0.125, ((0, 8), (1, 4)))
    in_bc = scatter_about(arg_keys[8], (D, 2 * N), D ** -0.5, 0.125, ((0, 8),))
    in_dt = scatter_about(arg_keys[9], (D, H), D ** -0.5, 0.125, ((0, 8), (1, 4)))
    out_t = scatter_about(arg_keys[10], (D, DI), DI ** -0.5, 0.078125, ((0, 8), (1, 4)))
    lm_head = draw_lm_head(jax.random.fold_in(arg_keys[22], 71), 0)
    conv_wx = scatter_about(arg_keys[12], (KCONV, DI), KCONV ** -0.5, 3.0, ((1, 4),), jnp.float32)
    conv_bx = scatter_about(arg_keys[13], (DI,), 0.3, 1.5, ((0, 4),), jnp.float32)
    conv_wbc = scatter_about(arg_keys[14], (KCONV, 2 * N), KCONV ** -0.5, 3.0, (), jnp.float32)
    conv_bbc = scatter_about(arg_keys[15], (2 * N,), 0.3, 1.5, (), jnp.float32)
    dt_bias = jnp.clip(-4.0 + 3.0 * jax.random.uniform(arg_keys[16], (H,), jnp.float32) ** level_of(arg_keys[16], (H,), ((0, 4),), -0.2, 0.2), -4.0, -1.0)
    a_log = jnp.clip(2.77 * jax.random.uniform(arg_keys[17], (H,), jnp.float32) ** level_of(arg_keys[17], (H,), ((0, 4),), -0.2, 0.2), 0.0, 2.77)
    skip_gain = jnp.clip(0.5 + 1.0 * jax.random.uniform(arg_keys[18], (H,), jnp.float32) ** level_of(arg_keys[18], (H,), ((0, 4),), -0.2, 0.2), 0.5, 1.5)
    norm_in = jnp.clip(1.0 + 0.1 * jax.random.normal(arg_keys[19], (D,), jnp.float32), 0.5, 1.5)
    norm_gain = jnp.clip(1.0 + 0.1 * jax.random.normal(arg_keys[20], (DI,), jnp.float32), 0.5, 1.5)
    final_gain = jnp.clip(1.0 + 0.1 * jax.random.normal(arg_keys[21], (D,), jnp.float32), 0.5, 1.5)
    return {"hidden_in": hidden_in, "ssm_state": ssm_state, "conv_x_state": conv_x_state, "conv_bc_state": conv_bc_state, "token_ids": token_ids, "ref_logits": ref_logits, "in_z": in_z, "in_x": in_x, "in_bc": in_bc, "in_dt": in_dt, "out_t": out_t, "lm_head": lm_head, "conv_wx": conv_wx, "conv_bx": conv_bx, "conv_wbc": conv_wbc, "conv_bbc": conv_bbc, "dt_bias": dt_bias, "a_log": a_log, "skip_gain": skip_gain, "norm_in": norm_in, "norm_gain": norm_gain, "final_gain": final_gain}


EPSILON = 1e-05

def rms_norm(values, gain):
    return values * lax.rsqrt(lax.optimization_barrier(jnp.mean(values * values, axis=-1, keepdims=True)) + EPSILON) * gain

def causal_conv(history, newest, taps, offset):
    window = jnp.concatenate([history, newest[:, None, :]], axis=1).astype(jnp.float32)
    return jax.nn.silu(lax.optimization_barrier(jnp.sum(window * taps[None, :, :], axis=1)) + offset)

def reference(hidden_in, ssm_state, conv_x_state, conv_bc_state, token_ids, ref_logits, in_z, in_x, in_bc, in_dt, out_t, lm_head, conv_wx, conv_bx, conv_wbc, conv_bbc, dt_bias, a_log, skip_gain, norm_in, norm_gain, final_gain):
    stream_in = hidden_in.astype(jnp.float32)
    normed = rms_norm(stream_in, norm_in).astype(jnp.bfloat16)
    gate_branch = jnp.dot(normed, in_z, preferred_element_type=jnp.float32).astype(jnp.bfloat16)
    x_branch = jnp.dot(normed, in_x, preferred_element_type=jnp.float32).astype(jnp.bfloat16)
    bc_branch = jnp.dot(normed, in_bc, preferred_element_type=jnp.float32).astype(jnp.bfloat16)
    step_raw = jnp.dot(normed, in_dt, preferred_element_type=jnp.float32).astype(jnp.bfloat16)
    x_conv = causal_conv(conv_x_state, x_branch, conv_wx, conv_bx)
    bc_conv = causal_conv(conv_bc_state, bc_branch, conv_wbc, conv_bbc)
    b_vals = bc_conv[:, :N]
    c_vals = bc_conv[:, N:]
    step = jax.nn.softplus(step_raw.astype(jnp.float32) + dt_bias)
    decay = jnp.exp(-step * jnp.exp(a_log))
    seq_count = x_conv.shape[0]
    x_heads = x_conv.reshape(seq_count, H, P_SIZE)
    inflow = (step[:, :, None] * x_heads)[:, :, :, None] * b_vals[:, None, None, :]
    new_state = decay[:, :, None, None] * ssm_state + inflow
    ssm_out = jnp.einsum('shpn,sn->shp', new_state, c_vals, precision=lax.Precision.HIGHEST)
    ssm_out = (ssm_out + skip_gain[None, :, None] * x_heads).reshape(seq_count, H * P_SIZE)
    gated = ssm_out * jax.nn.silu(gate_branch.astype(jnp.float32))
    gated_out = rms_norm(gated, norm_gain).astype(jnp.bfloat16)
    mixed = lax.dot_general(gated_out, out_t, (((1,), (1,)), ((), ())), preferred_element_type=jnp.float32)
    final_hidden = rms_norm(stream_in + mixed, final_gain).astype(jnp.bfloat16)
    logits = lax.dot_general(final_hidden, lm_head, (((1,), (1,)), ((), ())), preferred_element_type=jnp.float32)
    lse_roll = jax.nn.logsumexp(logits, axis=-1)
    reference_rows = ref_logits.astype(jnp.float32)
    lse_ref = jax.nn.logsumexp(reference_rows, axis=-1)
    log_ref = reference_rows - lse_ref[:, None]
    divergence = lax.optimization_barrier(jnp.sum(jnp.exp(log_ref) * (log_ref - (logits - lse_roll[:, None])), axis=-1))
    picked = jnp.take_along_axis(logits, token_ids[:, None].astype(jnp.int32), axis=1)[:, 0]
    token_logprob = picked - lse_roll
    return (new_state, divergence, token_logprob, in_z, in_x, in_bc, in_dt, out_t)
```

```python
import functools

import jax
import jax.numpy as jnp
from jax import lax
from jax.experimental import pallas as pl
from jax.experimental.pallas import tpu as pltpu
from jax.sharding import PartitionSpec as P

P_SIZE = 64
EPSILON = 1e-05
AHEAD = 2
PIECES = 5
PARTS = 5
MESH = pl.DeviceIdType.MESH


def flip(value, mask):
    bit = 1
    while bit <= mask:
        if mask & bit:
            value = value + bit * (1 - 2 * ((value // bit) % 2))
        bit *= 2
    return value


def greet(groups, heads):
    barrier = pltpu.get_barrier_semaphore()
    group, head = lax.axis_index("group"), lax.axis_index("head")
    for j in range(1, groups):
        pl.semaphore_signal(barrier, inc=1, device_id={"group": (group + j) % groups}, device_id_type=MESH)
    for j in range(1, heads):
        pl.semaphore_signal(barrier, inc=1, device_id={"head": (head + j) % heads}, device_id_type=MESH)
    pl.semaphore_wait(barrier, groups - 1 + heads - 1)


class Links:
    def __init__(self):
        self.pending = []

    def send(self, src, dst, device, ssem, rsem):
        made = pltpu.make_async_remote_copy(
            src_ref=src, dst_ref=dst, send_sem=ssem, recv_sem=rsem, device_id=device, device_id_type=MESH)
        made.start()
        self.pending.append(made)
        return made

    def drain(self):
        for made in self.pending:
            made.wait_send()


class Bulk:
    def __init__(self, links, chips, units, send, recv, psend, precv):
        self.links, self.chips, self.units = links, chips, units
        self.sems, self.pair_sems = (send, recv), (psend, precv)
        group = lax.axis_index("group")
        self.chip, self.core = group // 2, group % 2
        self.relay = chips == 4
        self.far, self.near = {}, []
        self.next = 0
        for k in range(AHEAD):
            self.own(k)

    def rows(self, k, chip):
        src, _, first, count = self.units[k]
        start = (chip * 2 + self.core) * src.shape[0] + first
        return self.units[k][1].at[pl.ds(pl.multiple_of(start, 16), count)]

    def across(self, k, m, src, dst, slot):
        send, recv = self.sems
        device = {"group": flip(self.chip, m) * 2 + self.core}
        self.far[k, slot] = self.links.send(src, dst, device, send.at[k, slot], recv.at[k, slot])

    def hand(self, k, src, dst, slot):
        send, recv = self.pair_sems
        device = {"group": self.chip * 2 + 1 - self.core}
        self.near.append(self.links.send(src, dst, device, send.at[k, slot], recv.at[k, slot]))

    def own(self, k):
        src, _, first, count = self.units[k]
        src, dst = src.at[pl.ds(first, count)], self.rows(k, self.chip)
        for m in [1, 2] if self.relay else range(1, self.chips):
            self.across(k, m, src, dst, m)
        self.hand(k, src, dst, 0)

    def step(self):
        k = self.next
        self.next += 1
        order = range(1, self.chips)
        if self.relay:
            order = (1, 2) if k % 2 == 0 else (2, 1)
        for m in order:
            self.far[k, m].wait_recv()
            view = self.rows(k, flip(self.chip, m))
            if self.relay and m == order[0]:
                self.across(k, 3 - m, view, view, 3)
            self.hand(k, view, view, m)
        if k + AHEAD < len(self.units):
            self.own(k + AHEAD)
        if k:
            self.last(k - 1)

    def last(self, k):
        if self.relay:
            self.far[k, 3].wait_recv()
            view = self.rows(k, flip(self.chip, 3))
            self.hand(k, view, view, 3)

    def pump(self, count):
        for _ in range(count):
            if self.next < len(self.units):
                self.step()

    def finish(self):
        self.pump(len(self.units))
        self.last(len(self.units) - 1)
        for made in self.near:
            made.wait_recv()


def halves(column, lanes, first, split):
    high = column.astype(jnp.bfloat16).astype(jnp.float32)
    return jnp.where(lanes < split, high, column - high)


def rms_scale(mean_square):
    return lax.rsqrt(mean_square + EPSILON)


def silu(values):
    return values * jax.nn.sigmoid(values)


def window(values, first, width):
    wide = width + (-width % 128 or 128)
    span = wide + 128
    start = min(first // 128 * 128, values.shape[1] - span)
    return pltpu.roll(values[:, start:start + span], (start - first) % span, 1)[:, :wide]


def own_window(values, group, groups, width):
    chosen = window(values, 0, width)
    for p in range(1, groups):
        chosen = jnp.where(group == p, window(values, p * width, width), chosen)
    return chosen


def step_kernel(
    groups, heads, local_heads,
    hid_ref, cx_ref, cbc_ref, token_ref, refl_ref, dt_ref, small_ref,
    wx_ref, bx_ref, wbc_ref, bbc_ref, norm_in_ref, ngain_ref, fgain_ref,
    state_hbm, z_hbm, x_hbm, bc_hbm, out_hbm, lm_hbm,
    new_ref, z_all, x_all, bc_all, out_all, dt_all, result_ref,
    lm_ref, hsend, hall, ppairs, ppair_in, psum, psum_in, dt_pad, inflow_ref, b_ref, c_ref, decay_ref, y_ref,
    gall, mix, pairs, pair_in, sums, sums_in, square, square_in, squares_out, squares_in, stat,
    load, bsend, brecv, bpsend, bprecv, hsem, hrsem, dsem, drsem, qsem, qrsem, rsem, rrsem, gsem, grsem,
    msend, mrecv, psend, precv, ssend, srecv, tsend, trecv,
):
    f32, bf16 = jnp.float32, jnp.bfloat16
    chips = groups // 2
    group, head = lax.axis_index("group"), lax.axis_index("head")
    chip, core = group // 2, group % 2
    seqs, model = hid_ref.shape
    depth, inner = z_hbm.shape
    wide = hall.shape[2]
    half, rows = chips * seqs, groups * seqs
    vocab = lm_ref.shape[1]
    parts, width = pairs.shape[0], pairs.shape[3]
    state_size = b_ref.shape[2]
    links = Links()
    send = links.send
    slot_of = lambda g: (g % 2) * chips + g // 2
    mine = slot_of(group)
    other = {"group": chip * 2 + 1 - core}

    loads = []

    def fetch(src, dst):
        made = pltpu.make_async_copy(src, dst, load.at[len(loads)])
        made.start()
        loads.append(made)
        return made

    own_rows = pl.ds(pl.multiple_of(group * depth, 16), depth)
    have = [fetch(src, dst.at[own_rows]) for src, dst in
            ((z_hbm, z_all), (x_hbm, x_all), (bc_hbm, bc_all), (out_hbm, out_all))]
    have_state = fetch(state_hbm, new_ref)
    have_lm = fetch(lm_hbm, lm_ref)

    hid = hid_ref[...].astype(f32)
    mean_square = jnp.mean(hid * hid, axis=-1, keepdims=True)
    lanes = lax.broadcasted_iota(jnp.int32, (seqs, wide), 1)
    middle = (depth + wide) // 2
    square_halves = halves(mean_square, lanes, depth, middle)
    for p in range(groups):
        hsend[p] = jnp.where(lanes < depth, window(hid, p * depth, depth), square_halves).astype(bf16)
    dt_pad[...] = jnp.zeros_like(dt_pad)
    dt_pad[0:local_heads, 0:depth] = dt_ref[...]

    greet(groups, heads)
    first, dts = [], []
    for j in range(1, groups):
        peer = (group + j) % groups
        first.append(send(hsend.at[peer], hall.at[mine], {"group": peer}, hsem.at[j], hrsem.at[j]))
    dt_rows = dt_all.shape[1]
    for m in range(1, chips):
        dts.append(send(dt_pad.at[pl.ds(0, dt_rows)], dt_all.at[group], {"group": flip(chip, m) * 2 + core},
                        dsem.at[0, m], drsem.at[0, m]))
    dts.append(send(dt_pad.at[pl.ds(0, dt_rows)], dt_all.at[group], other, dsem.at[1, 0], drsem.at[1, 0]))
    piece = depth // PIECES
    units = [(bc_hbm, bc_all, 0, depth)]
    for src, dst in ((z_hbm, z_all), (x_hbm, x_all), (out_hbm, out_all)):
        units += [(src, dst, n * piece, piece) for n in range(PIECES)]
    bulk = Bulk(links, chips, units, bsend, brecv, bpsend, bprecv)

    hall[mine] = hsend[group]
    dt_all[group] = dt_pad[0:dt_rows]
    norm_gain = own_window(norm_in_ref[...][None, :], group, groups, depth)
    final_gain = own_window(fgain_ref[...][None, :], group, groups, depth)
    for made in have[:3]:
        made.wait()
    for made in first:
        made.wait_recv()
    hidden = hall[...].reshape(rows, wide).astype(f32)
    mean_square = hidden[:, depth:depth + 1] + hidden[:, middle:middle + 1]
    normed = (hidden * rms_scale(mean_square) * norm_gain).astype(bf16)[:, :depth]
    at = 0
    for weights in (z_all, x_all, bc_all):
        cols = weights.shape[1]
        made = jnp.dot(normed, weights[own_rows, :], preferred_element_type=f32).astype(bf16)
        ppairs[0, :, at:at + cols], ppairs[1, :, at:at + cols] = made[:half], made[half:]
        at += cols
    made = lax.dot_general(
        normed, dt_pad[:, 0:depth], (((1,), (1,)), ((), ())), preferred_element_type=f32).astype(bf16)
    ppairs[0, :, at:at + 128], ppairs[1, :, at:at + 128] = made[:half], made[half:]
    handed = send(ppairs.at[1 - core], ppair_in, other, qsem, qrsem)
    for m in range(1, chips):
        dts[m - 1].wait_recv()
        view = dt_all.at[flip(chip, m) * 2 + core]
        dts.append(send(view, view, other, dsem.at[1, m], drsem.at[1, m]))
    handed.wait_recv()
    summed = ppairs[core].astype(f32) + ppair_in[...].astype(f32)
    psum[...] = summed.astype(bf16).reshape(psum.shape)
    spread = []
    for m in range(1, chips):
        peer = flip(chip, m)
        spread.append(send(
            psum.at[peer], psum_in.at[m], {"group": peer * 2 + core}, rsem.at[m], rrsem.at[m]))
    psum_in[0] = psum[chip]
    bulk.pump(2)
    for made in spread:
        made.wait_recv()
    branch = jnp.sum(psum_in[...].astype(f32), axis=0).astype(bf16).astype(f32)

    def conv(history, newest, taps, offset):
        total = newest * taps[history.shape[0]:, :]
        for n in range(history.shape[0]):
            total += history[n].astype(f32) * taps[n:n + 1, :]
        return silu(total + offset[None, :])

    gate = branch[:, :inner]
    x_conv = conv(cx_ref[...], branch[:, inner:2 * inner], wx_ref[...], bx_ref[...])
    bc_conv = conv(cbc_ref[...], branch[:, 2 * inner:2 * inner + 2 * state_size], wbc_ref[...], bbc_ref[...])
    raw = branch[:, 2 * inner + 2 * state_size:] + small_ref[0:1, :]
    step = jnp.maximum(raw, 0.0) + jnp.log1p(jnp.exp(-jnp.abs(raw)))
    decay = jnp.exp(-step * jnp.exp(small_ref[1:2, :]))
    place = lax.broadcasted_iota(jnp.int32, (128, inner), 0) * P_SIZE
    lane = lax.broadcasted_iota(jnp.int32, (128, inner), 1)
    chosen = jnp.where((lane >= place) & (lane < place + P_SIZE), 1.0, 0.0)
    by_head = jnp.concatenate([step, jnp.broadcast_to(small_ref[2:3, :], (8, 128))], axis=0)
    by_column = jnp.dot(by_head, chosen, preferred_element_type=f32, precision=lax.Precision.HIGHEST)
    inflow = by_column[:seqs] * x_conv
    skip = by_column[seqs:seqs + 1] * x_conv
    for s in range(seqs):
        inflow_ref[s] = inflow[s:s + 1]
        b_ref[s] = bc_conv[s:s + 1, :state_size]
        c_ref[s] = bc_conv[s:s + 1, state_size:]
        decay_ref[s] = decay[s:s + 1]
    have_state.wait()

    def pair(row):
        high = row.astype(bf16).astype(f32)
        return high, row - high

    def one(s):
        high, low = pair(inflow_ref[s])
        b_high, b_low = pair(b_ref[s])
        place = lax.broadcasted_iota(jnp.int32, (16, inner), 0)
        left = jnp.where(place < 2, high, jnp.where(place < 4, low, 0.0)).astype(bf16)
        place = lax.broadcasted_iota(jnp.int32, (16, state_size), 0)
        right = jnp.where(place % 2 == 0, b_high, b_low).astype(bf16)
        flow = lax.dot_general(left, right, (((0,), (0,)), ((), ())), preferred_element_type=f32)
        decays = decay_ref[s]
        for h in range(local_heads):
            new_ref[s, h] = decays[:, h:h + 1] * new_ref[s, h] + flow[h * P_SIZE:(h + 1) * P_SIZE]
        new = new_ref[s].reshape(inner, state_size).astype(bf16)
        c = jnp.broadcast_to(c_ref[s], (16, state_size)).astype(bf16)
        y = lax.dot_general(c, new, (((1,), (1,)), ((), ())), preferred_element_type=f32)
        y_ref[s] = y[0:1]

    bulk.pump(1)
    for lo, hi in ((0, seqs // 2), (seqs // 2, seqs)):
        pl.loop(lo, hi)(one)
        bulk.pump(1)

    ssm_out = jnp.concatenate([y_ref[s] for s in range(seqs)], axis=0) + skip
    gall[mine] = (ssm_out * silu(gate)).astype(bf16)
    sent = [send(gall.at[mine], gall.at[mine], {"group": flip(chip, m) * 2 + core}, gsem.at[0, m], grsem.at[0, m])
            for m in range(1, chips)]
    near = [send(gall.at[mine], gall.at[mine], other, gsem.at[1, 0], grsem.at[1, 0])]
    bulk.pump(1)
    for m in range(1, chips):
        sent[m - 1].wait_recv()
        view = gall.at[core * chips + flip(chip, m)]
        near.append(send(view, view, other, gsem.at[1, m], grsem.at[1, m]))
    for made in near:
        made.wait_recv()
    have[3].wait()

    gated = gall[...].reshape(rows, inner).astype(f32)
    squares = jnp.sum(gated * gated, axis=-1, keepdims=True)
    scaled = (gated * ngain_ref[...][None, :]).astype(bf16)
    out_rows = out_all[own_rows, :]
    out_rows = jnp.concatenate([out_rows, jnp.zeros((wide - depth, inner), bf16)], axis=0)
    partial = lax.dot_general(scaled, out_rows, (((1,), (1,)), ((), ())), preferred_element_type=f32)
    lanes = lax.broadcasted_iota(jnp.int32, (rows, wide), 1)
    mix[0] = jnp.where(lanes < depth, partial, halves(squares, lanes, depth, middle)).astype(bf16)
    mixes = [
        send(mix.at[0], mix.at[j], {"head": (head + j) % heads}, msend.at[j], mrecv.at[j])
        for j in range(1, heads)
    ]
    bulk.pump(1)
    have_lm.wait()
    for made in mixes:
        made.wait_recv()
    total = jnp.sum(mix[...].astype(f32), axis=0)
    square_total = total[:, depth:depth + 1] + total[:, middle:middle + 1]
    stream = hidden + total * rms_scale(square_total / (inner * heads))
    stream = jnp.where(lanes < depth, stream, 0.0)
    final_squares = jnp.sum(stream * stream, axis=-1, keepdims=True)
    final = (stream * final_gain).astype(bf16)[:, :depth]
    tail_lanes = lax.broadcasted_iota(jnp.int32, (rows, 128), 1)
    packed = halves(jnp.broadcast_to(final_squares, (rows, 128)), tail_lanes, 0, 64).astype(bf16)
    square[0], square[1] = packed[:half], packed[half:]
    pair_sends = [send(square.at[1 - core], square_in, other, psend.at[parts], precv.at[parts])]
    last = []

    def out(source, target, t):
        for m in range(1, chips):
            peer = flip(chip, m)
            last.append(send(
                source.at[peer], target.at[m], {"group": peer * 2 + core}, ssend.at[t, m], srecv.at[t, m]))
        target[0] = source[chip]

    def join(t):
        pair_sends[t + 1].wait_recv()
        joined = pairs[t, core].astype(f32) + pair_in[t].astype(f32)
        sums[t] = joined.astype(bf16).reshape(chips, seqs, width)
        out(sums.at[t], sums_in.at[t], t)

    for t in range(parts):
        block = jnp.dot(
            final, lm_ref[:, t * width:(t + 1) * width], preferred_element_type=f32).astype(bf16)
        pairs[t, 0], pairs[t, 1] = block[:half], block[half:]
        pair_sends.append(send(pairs.at[t, 1 - core], pair_in.at[t], other, psend.at[t], precv.at[t]))
        if t == 0:
            pair_sends[0].wait_recv()
            rest = square[core].astype(f32) + square_in[...].astype(f32)
            rest = rest[:, 0:1] + rest[:, 64:65]
            split = halves(rest, lax.broadcasted_iota(jnp.int32, (half, 128), 1), 0, 64)
            squares_out[...] = split.astype(bf16).reshape(chips, seqs, 128)
            out(squares_out, squares_in, parts)
        else:
            join(t - 1)
    join(parts - 1)
    bulk.pump(2)
    for made in last:
        made.wait_recv()
    bulk.pump(1)

    square_sum = jnp.sum(squares_in[...].astype(f32), axis=0)
    mean_square = (square_sum[:, 0:1] + square_sum[:, 64:65]) / model
    logits = jnp.concatenate([jnp.sum(sums_in[t].astype(f32), axis=0) for t in range(parts)], axis=1)
    logits = logits * rms_scale(mean_square)
    reference = refl_ref[...].astype(f32)
    row = lax.broadcasted_iota(jnp.int32, (seqs, 128), 0)
    tokens = jnp.zeros((seqs, 128), jnp.int32)
    for s in range(seqs):
        tokens = jnp.where(row == s, token_ref[s], tokens)
    columns = lax.broadcasted_iota(jnp.int32, (seqs, vocab), 1) + head * vocab
    picked = jnp.sum(jnp.where(columns == tokens[:, 0:1], logits, 0.0), axis=-1, keepdims=True)
    top = jnp.max(logits, axis=-1, keepdims=True)
    ref_top = jnp.max(reference, axis=-1, keepdims=True)
    weights = jnp.exp(reference - ref_top)
    values = (
        top,
        jnp.sum(jnp.exp(logits - top), axis=-1, keepdims=True),
        ref_top,
        jnp.sum(weights, axis=-1, keepdims=True),
        jnp.sum(weights * (reference - logits), axis=-1, keepdims=True),
        picked,
    )
    slot = lax.broadcasted_iota(jnp.int32, (seqs, 128), 1)
    mine_values = jnp.zeros((seqs, 128), f32)
    for n, value in enumerate(values):
        mine_values = jnp.where(slot == n, value, mine_values)
    stat[0] = mine_values
    stats = [
        send(stat.at[0], stat.at[j], {"head": (head + j) % heads}, tsend.at[j], trecv.at[j])
        for j in range(1, heads)
    ]
    for made in stats:
        made.wait_recv()
    every = stat[...]
    pick = lambda n: every[:, :, n:n + 1]
    top = jnp.max(pick(0), axis=0)
    ref_top = jnp.max(pick(2), axis=0)
    factor = jnp.exp(pick(0) - top[None])
    ref_factor = jnp.exp(pick(2) - ref_top[None])
    roll_sum = jnp.sum(pick(1) * factor, axis=0)
    ref_sum = jnp.sum(pick(3) * ref_factor, axis=0)
    cross = jnp.sum(pick(4) * ref_factor, axis=0)
    picked = jnp.sum(pick(5), axis=0)
    lse_roll = top + jnp.log(roll_sum)
    lse_ref = ref_top + jnp.log(ref_sum)
    result_ref[...] = jnp.where(slot == 0, cross / ref_sum - lse_ref + lse_roll, picked - lse_roll)

    bulk.finish()
    for made in dts[chips - 1:]:
        made.wait_recv()
    links.drain()


def publish_kernel(count, *refs):
    ins, dt_ref, result_ref = refs[:count], refs[count], refs[count + 1]
    outs, dt_out, div_out, prob_out, sems = refs[count + 2:2 * count + 2], *refs[2 * count + 2:]
    made = []
    for n, (src, dst) in enumerate(zip(ins, outs)):
        size = src.shape[0] // 4
        for p in range(4):
            rows = pl.ds(p * size, size)
            made.append(pltpu.make_async_copy(src.at[rows], dst.at[rows], sems.at[n, p]))
            made[-1].start()
    local_heads, model = dt_out.shape
    groups = dt_ref.shape[0]
    depth = model // groups
    dt_out[...] = jnp.concatenate(
        [dt_ref[g].astype(jnp.float32)[:, :depth] for g in range(groups)], axis=1
    )[:local_heads].astype(dt_out.dtype)
    seqs = div_out.shape[1]
    result = result_ref[...]
    same = lax.broadcasted_iota(jnp.int32, (seqs, seqs), 0) == lax.broadcasted_iota(jnp.int32, (seqs, seqs), 1)
    for n, ref in enumerate((div_out, prob_out)):
        ref[...] = jnp.sum(jnp.where(same, result[:, n:n + 1], 0.0), axis=0, keepdims=True)
    for copy in made:
        copy.wait()


def shards(
    groups, heads,
    hidden_in, ssm_state, conv_x_state, conv_bc_state, token_ids, ref_logits,
    in_z, in_x, in_bc, in_dt, out_t, lm_head,
    conv_wx, conv_bx, conv_wbc, conv_bbc, dt_bias, a_log, skip_gain, norm_in, norm_gain, final_gain,
):
    seqs, model = hidden_in.shape
    depth, inner = in_z.shape
    local_heads = a_log.shape[0]
    state_size = ssm_state.shape[3]
    chips = groups // 2
    half, rows = chips * seqs, groups * seqs
    wide = depth + (-depth % 128 or 128)
    vocab = lm_head.shape[0]
    width = vocab // PARTS
    cols = 2 * inner + in_bc.shape[1] + 128
    dt_rows = -(-local_heads // 16) * 16
    small = jnp.pad(jnp.stack([dt_bias, a_log, skip_gain]), ((0, 5), (0, 128 - local_heads)))
    bf16, f32 = jnp.bfloat16, jnp.float32
    vmem, hbm = pl.BlockSpec(memory_space=pltpu.VMEM), pl.BlockSpec(memory_space=pltpu.HBM)
    smem, any_spec = pl.BlockSpec(memory_space=pltpu.SMEM), pl.BlockSpec(memory_space=pl.ANY)
    scratch = pltpu.VMEM
    dma = pltpu.SemaphoreType.DMA
    units = 3 * PIECES + 1
    slots = max(chips, 4)
    gathered = [(groups * depth, w.shape[1]) for w in (in_z, in_x, in_bc, out_t)]
    made = pl.pallas_call(
        functools.partial(step_kernel, groups, heads, local_heads),
        out_shape=[pltpu.VMEM(ssm_state.shape, f32)] + [pltpu.VMEM(shape, bf16) for shape in gathered]
        + [pltpu.VMEM((groups, dt_rows, wide), bf16), pltpu.VMEM((seqs, 128), f32)],
        in_specs=[vmem] * 3 + [smem] + [vmem] * 10 + [hbm] * 6,
        out_specs=[vmem] * 7,
        scratch_shapes=[
            scratch((depth, vocab), bf16),
            scratch((groups, seqs, wide), bf16), scratch((groups, seqs, wide), bf16),
            scratch((2, half, cols), bf16), scratch((half, cols), bf16),
            scratch((chips, seqs, cols), bf16), scratch((chips, seqs, cols), bf16),
            scratch((128, wide), bf16),
            scratch((seqs, 1, inner), f32), scratch((seqs, 1, state_size), f32), scratch((seqs, 1, state_size), f32),
            scratch((seqs, 1, 128), f32), scratch((seqs, 1, inner), f32),
            scratch((groups, seqs, inner), bf16),
            scratch((heads, rows, wide), bf16),
            scratch((PARTS, 2, half, width), bf16), scratch((PARTS, half, width), bf16),
            scratch((PARTS, chips, seqs, width), bf16), scratch((PARTS, chips, seqs, width), bf16),
            scratch((2, half, 128), bf16), scratch((half, 128), bf16),
            scratch((chips, seqs, 128), bf16), scratch((chips, seqs, 128), bf16),
            scratch((heads, seqs, 128), f32),
            dma((6,)), dma((units, slots)), dma((units, slots)), dma((units, slots)), dma((units, slots)),
            dma((groups,)), dma((groups,)), dma((2, chips)), dma((2, chips)), dma, dma,
            dma((chips,)), dma((chips,)), dma((2, chips)), dma((2, chips)),
            dma((heads,)), dma((heads,)), dma((PARTS + 1,)), dma((PARTS + 1,)),
            dma((PARTS + 1, chips)), dma((PARTS + 1, chips)), dma((heads,)), dma((heads,)),
        ],
        compiler_params=pltpu.CompilerParams(
            collective_id=0, has_side_effects=True, vmem_limit_bytes=32 * 1024 * 1024),
        name="step",
    )(
        hidden_in, conv_x_state.transpose(1, 0, 2), conv_bc_state.transpose(1, 0, 2), token_ids, ref_logits, in_dt.T,
        small, conv_wx, conv_bx, conv_wbc, conv_bbc, norm_in, norm_gain, final_gain,
        ssm_state, in_z, in_x, in_bc, out_t, lm_head.T,
    )
    new_state, *rolls, dt_all, result = made
    count = len(rolls) + 1
    published = pl.pallas_call(
        functools.partial(publish_kernel, count),
        out_shape=[jax.ShapeDtypeStruct(ssm_state.shape, f32)] + [jax.ShapeDtypeStruct(v, bf16) for v in gathered]
        + [jax.ShapeDtypeStruct((local_heads, model), bf16)] + [jax.ShapeDtypeStruct((1, seqs), f32)] * 2,
        in_specs=[any_spec] * count + [vmem] * 2,
        out_specs=[any_spec] * count + [vmem] * 3,
        scratch_shapes=[dma((count, 4))],
        compiler_params=pltpu.CompilerParams(vmem_limit_bytes=1 * 1024 * 1024),
        name="publish",
    )(new_state, *rolls, dt_all, result)
    new_state, roll_z, roll_x, roll_bc, roll_out, roll_dt, divergence, logprob = published
    return new_state, divergence[0], logprob[0], roll_z, roll_x, roll_bc, roll_dt.T, roll_out


def solution(mesh):
    return jax.shard_map(
        functools.partial(shards, mesh.shape["group"], mesh.shape["head"]),
        mesh=mesh,
        in_specs=(
            P("group", None),
            P("group", "head", None, None),
            P("group", None, "head"),
            P("group", None, None),
            P("group"),
            P("group", "head"),
            P("group", "head"),
            P("group", "head"),
            P("group", None),
            P("group", "head"),
            P("group", "head"),
            P("head", "group"),
            P(None, "head"),
            P("head"),
            P(),
            P(),
            P("head"),
            P("head"),
            P("head"),
            P(),
            P("head"),
            P(),
        ),
        out_specs=(
            P("group", "head", None, None),
            P("group"),
            P("group"),
            P(None, "head"),
            P(None, "head"),
            P(),
            P(None, "head"),
            P(None, "head"),
        ),
        check_vma=False,
    )
```

```python
import functools

import jax
import jax.numpy as jnp
from jax import lax
from jax.experimental import pallas as pl
from jax.experimental.pallas import tpu as pltpu
from jax.sharding import PartitionSpec as P

P_SIZE = 64
EPSILON = 1e-05
AHEAD = 3
PIECES = 5
PARTS = 5
MESH = pl.DeviceIdType.MESH


def flip(value, mask):
    bit = 1
    while bit <= mask:
        if mask & bit:
            value = value + bit * (1 - 2 * ((value // bit) % 2))
        bit *= 2
    return value


def greet(groups, heads):
    barrier = pltpu.get_barrier_semaphore()
    group, head = lax.axis_index("group"), lax.axis_index("head")
    for j in range(1, groups):
        pl.semaphore_signal(barrier, inc=1, device_id={"group": (group + j) % groups}, device_id_type=MESH)
    for j in range(1, heads):
        pl.semaphore_signal(barrier, inc=1, device_id={"head": (head + j) % heads}, device_id_type=MESH)
    pl.semaphore_wait(barrier, groups - 1 + heads - 1)


class Links:
    def __init__(self):
        self.pending = []

    def send(self, src, dst, device, ssem, rsem):
        made = pltpu.make_async_remote_copy(
            src_ref=src, dst_ref=dst, send_sem=ssem, recv_sem=rsem, device_id=device, device_id_type=MESH)
        made.start()
        self.pending.append(made)
        return made

    def drain(self):
        for made in self.pending:
            made.wait_send()


class Bulk:
    def __init__(self, links, chips, units, send, recv, psend, precv):
        self.links, self.chips, self.units = links, chips, units
        self.sems, self.pair_sems = (send, recv), (psend, precv)
        group = lax.axis_index("group")
        self.chip, self.core = group // 2, group % 2
        self.relay = chips == 4
        self.peers = (1, 2) if self.relay else range(1, chips)
        self.far, self.near = {}, {}
        self.next, self.fed = 0, 0
        self.feed(2)

    def feed(self, ahead):
        while self.fed < min(self.next + ahead, len(self.units)):
            self.own(self.fed)
            self.fed += 1

    def rows(self, k, chip, part=None):
        src, dst, first, count = self.units[k]
        if part is not None:
            count = count // 2
            first = first + part * count
        group = chip * 2 + self.core
        if len(dst.shape) == 3:
            return dst.at[group, pl.ds(first, count)]
        return dst.at[pl.ds(pl.multiple_of(group * src.shape[0] + first, 16), count)]

    def across(self, k, m, src, dst, slot):
        send, recv = self.sems
        device = {"group": flip(self.chip, m) * 2 + self.core}
        self.far[k, slot] = self.links.send(src, dst, device, send.at[k, slot], recv.at[k, slot])

    def hand(self, k, src, dst, slot):
        send, recv = self.pair_sems
        device = {"group": self.chip * 2 + 1 - self.core}
        self.near.setdefault(k, []).append(self.links.send(src, dst, device, send.at[k, slot], recv.at[k, slot]))

    def own(self, k):
        src, _, first, count = self.units[k]
        src, dst = src.at[pl.ds(first, count)], self.rows(k, self.chip)
        for m in self.peers:
            self.across(k, m, src, dst, m)
        self.hand(k, src, dst, 0)

    def step(self, ahead):
        k = self.next
        self.next += 1
        for m in self.peers:
            self.far[k, m].wait_recv()
            for by, part, slot in self.relays(k):
                if by == m:
                    view = self.rows(k, flip(self.chip, m), part)
                    self.across(k, 3 - m, view, view, slot)
            view = self.rows(k, flip(self.chip, m))
            self.hand(k, view, view, m)
        self.feed(ahead)
        if k:
            self.last(k - 1)

    def relays(self, k):
        if not self.relay:
            return []
        return [(1, 0, 3), (2, 1, 4)] if self.units[k][3] % 32 == 0 else [(1, None, 3)]

    def last(self, k):
        for _, part, slot in self.relays(k):
            self.far[k, slot].wait_recv()
            view = self.rows(k, flip(self.chip, 3), part)
            self.hand(k, view, view, slot)

    def pump(self, count, ahead=AHEAD):
        for _ in range(count):
            if self.next < len(self.units):
                self.step(ahead)

    def finish(self):
        self.pump(len(self.units))
        self.last(len(self.units) - 1)
        for k in range(len(self.units)):
            self.arrive(k)

    def arrive(self, k):
        for made in self.near.pop(k, []):
            made.wait_recv()


def halves(column, lanes, first, split):
    high = column.astype(jnp.bfloat16).astype(jnp.float32)
    return jnp.where(lanes < split, high, column - high)


def rms_scale(mean_square):
    return lax.rsqrt(mean_square + EPSILON)


def silu(values):
    return values * jax.nn.sigmoid(values)


def window(values, first, width):
    wide = width + (-width % 128 or 128)
    span = wide + 128
    start = min(first // 128 * 128, values.shape[1] - span)
    return pltpu.roll(values[:, start:start + span], (start - first) % span, 1)[:, :wide]


def own_window(values, group, groups, width):
    chosen = window(values, 0, width)
    for p in range(1, groups):
        chosen = jnp.where(group == p, window(values, p * width, width), chosen)
    return chosen


def step_kernel(
    groups, heads, local_heads,
    hid_ref, cx_ref, cbc_ref, token_ref, refl_ref, dt_ref, bias_ref, rate_ref, skip_ref,
    wx_ref, bx_ref, wbc_ref, bbc_ref, norm_in_ref, ngain_ref, fgain_ref,
    state_hbm, z_hbm, x_hbm, bc_hbm, out_hbm, lm_hbm,
    new_ref, z_all, x_all, bc_all, out_all, dt_all, result_ref,
    bc_own, small_ref, lm_ref, hsend, hall, ppairs, ppair_in, psum, psum_in, dt_pad, inflow_ref, b_ref, c_ref, decay_ref, y_ref,
    gall, mix, pairs, pair_in, sums, sums_in, square, square_in, squares_out, squares_in, stat,
    load, bsend, brecv, bpsend, bprecv, hsem, hrsem, dsem, drsem, qsem, qrsem, rsem, rrsem, gsem, grsem,
    msend, mrecv, psend, precv, ssend, srecv, tsend, trecv, zsem, zrsem, ysem, yrsem,
):
    f32, bf16 = jnp.float32, jnp.bfloat16
    chips = groups // 2
    group, head = lax.axis_index("group"), lax.axis_index("head")
    chip, core = group // 2, group % 2
    seqs, model = hid_ref.shape
    depth, inner = z_hbm.shape
    wide = hall.shape[2]
    half, rows = chips * seqs, groups * seqs
    vocab = lm_ref.shape[1]
    parts, width = pairs.shape[0], pairs.shape[3]
    state_size = b_ref.shape[2]
    links = Links()
    send = links.send
    slot_of = lambda g: (g % 2) * chips + g // 2
    mine = slot_of(group)
    other = {"group": chip * 2 + 1 - core}

    loads = []

    def fetch(src, dst):
        made = pltpu.make_async_copy(src, dst, load.at[len(loads)])
        made.start()
        loads.append(made)
        return made

    own_rows = pl.ds(pl.multiple_of(group * depth, 16), depth)
    have = [fetch(src, dst) for src, dst in (
        (z_hbm, z_all.at[own_rows]), (x_hbm, x_all.at[own_rows]),
        (bc_hbm, bc_own), (out_hbm, out_all.at[own_rows]))]
    split = depth % (16 * heads) == 0
    share_rows = depth // heads if split else depth
    share_at = pl.multiple_of(head * share_rows, 16) if split else 0
    have_share = fetch(bc_hbm.at[pl.ds(share_at, share_rows)], bc_all.at[group, pl.ds(share_at, share_rows)])
    have_state = fetch(state_hbm, new_ref)
    have_lm = fetch(lm_hbm, lm_ref)

    hid = hid_ref[...].astype(f32)
    mean_square = jnp.mean(hid * hid, axis=-1, keepdims=True)
    lanes = lax.broadcasted_iota(jnp.int32, (seqs, wide), 1)
    middle = (depth + wide) // 2
    square_halves = halves(mean_square, lanes, depth, middle)
    for p in range(groups):
        hsend[p] = jnp.where(lanes < depth, window(hid, p * depth, depth), square_halves).astype(bf16)
    dt_pad[...] = jnp.zeros_like(dt_pad)
    dt_pad[0:local_heads, 0:depth] = dt_ref[...]
    small_ref[...] = jnp.zeros_like(small_ref)
    for n, ref in enumerate((bias_ref, rate_ref, skip_ref)):
        small_ref[n:n + 1, 0:local_heads] = ref[...][None, :]

    greet(groups, heads)
    first, dts = [], []
    for j in range(1, groups):
        peer = (group + j) % groups
        first.append(send(hsend.at[peer], hall.at[mine], {"group": peer}, hsem.at[j], hrsem.at[j]))
    dt_rows = dt_all.shape[1]
    for m in range(1, chips):
        dts.append(send(dt_pad.at[pl.ds(0, dt_rows)], dt_all.at[group], {"group": flip(chip, m) * 2 + core},
                        dsem.at[0, m], drsem.at[0, m]))
    dts.append(send(dt_pad.at[pl.ds(0, dt_rows)], dt_all.at[group], other, dsem.at[1, 0], drsem.at[1, 0]))
    piece = depth // PIECES
    units = [(bc_hbm, bc_all, share_at, share_rows)]
    for src, dst in ((z_hbm, z_all), (x_hbm, x_all), (out_hbm, out_all)):
        units += [(src, dst, n * piece, piece) for n in range(PIECES)]
    bulk = Bulk(links, chips, units, bsend, brecv, bpsend, bprecv)

    hall[mine] = hsend[group]
    dt_all[group] = dt_pad[0:dt_rows]
    norm_gain = own_window(norm_in_ref[...][None, :], group, groups, depth)
    final_gain = own_window(fgain_ref[...][None, :], group, groups, depth)
    for made in have[:3]:
        made.wait()
    for made in first:
        made.wait_recv()
    hidden = hall[...].reshape(rows, wide).astype(f32)
    mean_square = hidden[:, depth:depth + 1] + hidden[:, middle:middle + 1]
    normed = (hidden * rms_scale(mean_square) * norm_gain).astype(bf16)[:, :depth]
    at = 0
    for weights in (z_all[own_rows, :], x_all[own_rows, :], bc_own[...]):
        cols = weights.shape[1]
        made = jnp.dot(normed, weights, preferred_element_type=f32).astype(bf16)
        ppairs[0, :, at:at + cols], ppairs[1, :, at:at + cols] = made[:half], made[half:]
        at += cols
    made = lax.dot_general(
        normed, dt_pad[:, 0:depth], (((1,), (1,)), ((), ())), preferred_element_type=f32).astype(bf16)
    ppairs[0, :, at:at + 128], ppairs[1, :, at:at + 128] = made[:half], made[half:]
    handed = send(ppairs.at[1 - core], ppair_in, other, qsem, qrsem)
    for m in range(1, chips):
        dts[m - 1].wait_recv()
        view = dt_all.at[flip(chip, m) * 2 + core]
        dts.append(send(view, view, other, dsem.at[1, m], drsem.at[1, m]))
    handed.wait_recv()
    summed = ppairs[core].astype(f32) + ppair_in[...].astype(f32)
    psum[...] = summed.astype(bf16).reshape(psum.shape)
    spread = []
    for m in range(1, chips):
        peer = flip(chip, m)
        spread.append(send(
            psum.at[peer], psum_in.at[m], {"group": peer * 2 + core}, rsem.at[m], rrsem.at[m]))
    psum_in[0] = psum[chip]
    bulk.pump(1)
    for made in spread:
        made.wait_recv()
    branch = jnp.sum(psum_in[...].astype(f32), axis=0).astype(bf16).astype(f32)

    def conv(history, newest, taps, offset):
        total = newest * taps[history.shape[0]:, :]
        for n in range(history.shape[0]):
            total += history[n].astype(f32) * taps[n:n + 1, :]
        return silu(total + offset[None, :])

    gate = branch[:, :inner]
    x_conv = conv(cx_ref[...], branch[:, inner:2 * inner], wx_ref[...], bx_ref[...])
    bc_conv = conv(cbc_ref[...], branch[:, 2 * inner:2 * inner + 2 * state_size], wbc_ref[...], bbc_ref[...])
    raw = branch[:, 2 * inner + 2 * state_size:] + small_ref[0:1, :]
    step = jnp.maximum(raw, 0.0) + jnp.log1p(jnp.exp(-jnp.abs(raw)))
    decay = jnp.exp(-step * jnp.exp(small_ref[1:2, :]))
    place = lax.broadcasted_iota(jnp.int32, (128, inner), 0) * P_SIZE
    lane = lax.broadcasted_iota(jnp.int32, (128, inner), 1)
    chosen = jnp.where((lane >= place) & (lane < place + P_SIZE), 1.0, 0.0)
    by_head = jnp.concatenate([step, jnp.broadcast_to(small_ref[2:3, :], (8, 128))], axis=0)
    by_column = jnp.dot(by_head, chosen, preferred_element_type=f32, precision=lax.Precision.HIGHEST)
    inflow = by_column[:seqs] * x_conv
    skip = by_column[seqs:seqs + 1] * x_conv
    for s in range(seqs):
        inflow_ref[s] = inflow[s:s + 1]
        b_ref[s] = bc_conv[s:s + 1, :state_size]
        c_ref[s] = bc_conv[s:s + 1, state_size:]
        decay_ref[s] = decay[s:s + 1]
    have_state.wait()

    def pair(row):
        high = row.astype(bf16).astype(f32)
        return high, row - high

    def one(s):
        high, low = pair(inflow_ref[s])
        b_high, b_low = pair(b_ref[s])
        place = lax.broadcasted_iota(jnp.int32, (16, inner), 0)
        left = jnp.where(place < 2, high, jnp.where(place < 4, low, 0.0)).astype(bf16)
        place = lax.broadcasted_iota(jnp.int32, (16, state_size), 0)
        right = jnp.where(place % 2 == 0, b_high, b_low).astype(bf16)
        flow = lax.dot_general(left, right, (((0,), (0,)), ((), ())), preferred_element_type=f32)
        decays = decay_ref[s]
        for h in range(local_heads):
            new_ref[s, h] = decays[:, h:h + 1] * new_ref[s, h] + flow[h * P_SIZE:(h + 1) * P_SIZE]
        new = new_ref[s].reshape(inner, state_size).astype(bf16)
        c = jnp.broadcast_to(c_ref[s], (16, state_size)).astype(bf16)
        y = lax.dot_general(c, new, (((1,), (1,)), ((), ())), preferred_element_type=f32)
        y_ref[s] = y[0:1]

    bulk.pump(1)
    passed, crossed = [], []
    have_share.wait()
    if split:
        bulk.arrive(0)
        for j in range(1, heads):
            view = bc_all.at[pl.ds(core * chips, chips), pl.ds(share_at, share_rows)]
            crossed.append(send(view, view, {"head": (head + j) % heads}, zsem.at[j], zrsem.at[j]))
    for n in range(4):
        pl.loop(n * seqs // 4, (n + 1) * seqs // 4)(one)
        bulk.pump(1, 3 if n < 3 else 2)
    for j, made in enumerate(crossed, 1):
        made.wait_recv()
        first_row = pl.multiple_of((head - j + heads) % heads * share_rows, 16)
        view = bc_all.at[pl.ds(core * chips, chips), pl.ds(first_row, share_rows)]
        passed.append(send(view, view, other, ysem.at[j], yrsem.at[j]))

    ssm_out = jnp.concatenate([y_ref[s] for s in range(seqs)], axis=0) + skip
    gall[mine] = (ssm_out * silu(gate)).astype(bf16)
    sent = [send(gall.at[mine], gall.at[mine], {"group": flip(chip, m) * 2 + core}, gsem.at[0, m], grsem.at[0, m])
            for m in range(1, chips)]
    near = [send(gall.at[mine], gall.at[mine], other, gsem.at[1, 0], grsem.at[1, 0])]
    bulk.pump(1)
    for m in range(1, chips):
        sent[m - 1].wait_recv()
        view = gall.at[core * chips + flip(chip, m)]
        near.append(send(view, view, other, gsem.at[1, m], grsem.at[1, m]))
    for made in near:
        made.wait_recv()
    have[3].wait()

    gated = gall[...].reshape(rows, inner).astype(f32)
    squares = jnp.sum(gated * gated, axis=-1, keepdims=True)
    scaled = (gated * ngain_ref[...][None, :]).astype(bf16)
    out_rows = out_all[own_rows, :]
    out_rows = jnp.concatenate([out_rows, jnp.zeros((wide - depth, inner), bf16)], axis=0)
    partial = lax.dot_general(scaled, out_rows, (((1,), (1,)), ((), ())), preferred_element_type=f32)
    lanes = lax.broadcasted_iota(jnp.int32, (rows, wide), 1)
    mix[0] = jnp.where(lanes < depth, partial, halves(squares, lanes, depth, middle)).astype(bf16)
    mixes = [
        send(mix.at[0], mix.at[j], {"head": (head + j) % heads}, msend.at[j], mrecv.at[j])
        for j in range(1, heads)
    ]
    bulk.pump(1, 4)
    have_lm.wait()
    for made in mixes:
        made.wait_recv()
    total = jnp.sum(mix[...].astype(f32), axis=0)
    square_total = total[:, depth:depth + 1] + total[:, middle:middle + 1]
    stream = hidden + total * rms_scale(square_total / (inner * heads))
    stream = jnp.where(lanes < depth, stream, 0.0)
    final_squares = jnp.sum(stream * stream, axis=-1, keepdims=True)
    final = (stream * final_gain).astype(bf16)[:, :depth]
    tail_lanes = lax.broadcasted_iota(jnp.int32, (rows, 128), 1)
    packed = halves(jnp.broadcast_to(final_squares, (rows, 128)), tail_lanes, 0, 64).astype(bf16)
    square[0], square[1] = packed[:half], packed[half:]
    pair_sends = [send(square.at[1 - core], square_in, other, psend.at[parts], precv.at[parts])]
    last = []

    def out(source, target, t):
        for m in range(1, chips):
            peer = flip(chip, m)
            last.append(send(
                source.at[peer], target.at[m], {"group": peer * 2 + core}, ssend.at[t, m], srecv.at[t, m]))
        target[0] = source[chip]

    def join(t):
        pair_sends[t + 1].wait_recv()
        joined = pairs[t, core].astype(f32) + pair_in[t].astype(f32)
        sums[t] = joined.astype(bf16).reshape(chips, seqs, width)
        out(sums.at[t], sums_in.at[t], t)

    for t in range(parts):
        block = jnp.dot(
            final, lm_ref[:, t * width:(t + 1) * width], preferred_element_type=f32).astype(bf16)
        pairs[t, 0], pairs[t, 1] = block[:half], block[half:]
        pair_sends.append(send(pairs.at[t, 1 - core], pair_in.at[t], other, psend.at[t], precv.at[t]))
        if t == 0:
            pair_sends[0].wait_recv()
            rest = square[core].astype(f32) + square_in[...].astype(f32)
            rest = rest[:, 0:1] + rest[:, 64:65]
            split = halves(rest, lax.broadcasted_iota(jnp.int32, (half, 128), 1), 0, 64)
            squares_out[...] = split.astype(bf16).reshape(chips, seqs, 128)
            out(squares_out, squares_in, parts)
        else:
            join(t - 1)
    join(parts - 1)
    bulk.pump(2)
    for made in last:
        made.wait_recv()
    bulk.pump(1)

    square_sum = jnp.sum(squares_in[...].astype(f32), axis=0)
    mean_square = (square_sum[:, 0:1] + square_sum[:, 64:65]) / model
    logits = jnp.concatenate([jnp.sum(sums_in[t].astype(f32), axis=0) for t in range(parts)], axis=1)
    logits = logits * rms_scale(mean_square)
    reference = refl_ref[...].astype(f32)
    row = lax.broadcasted_iota(jnp.int32, (seqs, 128), 0)
    tokens = jnp.zeros((seqs, 128), jnp.int32)
    for s in range(seqs):
        tokens = jnp.where(row == s, token_ref[s], tokens)
    columns = lax.broadcasted_iota(jnp.int32, (seqs, vocab), 1) + head * vocab
    picked = jnp.sum(jnp.where(columns == tokens[:, 0:1], logits, 0.0), axis=-1, keepdims=True)
    top = jnp.max(logits, axis=-1, keepdims=True)
    ref_top = jnp.max(reference, axis=-1, keepdims=True)
    weights = jnp.exp(reference - ref_top)
    values = (
        top,
        jnp.sum(jnp.exp(logits - top), axis=-1, keepdims=True),
        ref_top,
        jnp.sum(weights, axis=-1, keepdims=True),
        jnp.sum(weights * (reference - logits), axis=-1, keepdims=True),
        picked,
    )
    slot = lax.broadcasted_iota(jnp.int32, (seqs, 128), 1)
    mine_values = jnp.zeros((seqs, 128), f32)
    for n, value in enumerate(values):
        mine_values = jnp.where(slot == n, value, mine_values)
    stat[0] = mine_values
    stats = [
        send(stat.at[0], stat.at[j], {"head": (head + j) % heads}, tsend.at[j], trecv.at[j])
        for j in range(1, heads)
    ]
    for made in stats:
        made.wait_recv()
    every = stat[...]
    pick = lambda n: every[:, :, n:n + 1]
    top = jnp.max(pick(0), axis=0)
    ref_top = jnp.max(pick(2), axis=0)
    factor = jnp.exp(pick(0) - top[None])
    ref_factor = jnp.exp(pick(2) - ref_top[None])
    roll_sum = jnp.sum(pick(1) * factor, axis=0)
    ref_sum = jnp.sum(pick(3) * ref_factor, axis=0)
    cross = jnp.sum(pick(4) * ref_factor, axis=0)
    picked = jnp.sum(pick(5), axis=0)
    lse_roll = top + jnp.log(roll_sum)
    lse_ref = ref_top + jnp.log(ref_sum)
    result_ref[...] = jnp.where(slot == 0, cross / ref_sum - lse_ref + lse_roll, picked - lse_roll)

    bulk.finish()
    for made in passed:
        made.wait_recv()
    for made in dts[chips - 1:]:
        made.wait_recv()
    links.drain()


def publish_kernel(count, *refs):
    ins, dt_ref, result_ref = refs[:count], refs[count], refs[count + 1]
    outs, smalls, (sems, *held) = refs[count + 2:2 * count + 2], refs[2 * count + 2:2 * count + 5], refs[2 * count + 5:]
    dt_out, div_out, prob_out = held
    made = []
    for n, (src, dst) in enumerate(zip(ins, outs)):
        size = src.shape[0] // 4
        for p in range(4):
            rows = pl.ds(p * size, size)
            made.append(pltpu.make_async_copy(src.at[rows], dst.at[rows], sems.at[n, p]))
            made[-1].start()
    local_heads, model = dt_out.shape
    groups = dt_ref.shape[0]
    depth = model // groups
    dt_out[...] = jnp.concatenate(
        [dt_ref[g].astype(jnp.float32)[:, :depth] for g in range(groups)], axis=1
    )[:local_heads].astype(dt_out.dtype)
    seqs = div_out.shape[1]
    result = result_ref[...]
    same = lax.broadcasted_iota(jnp.int32, (seqs, seqs), 0) == lax.broadcasted_iota(jnp.int32, (seqs, seqs), 1)
    for n, ref in enumerate((div_out, prob_out)):
        ref[...] = jnp.sum(jnp.where(same, result[:, n:n + 1], 0.0), axis=0, keepdims=True)
    for n, (src, dst) in enumerate(zip(held, smalls)):
        made.append(pltpu.make_async_copy(src, dst, sems.at[count, n]))
        made[-1].start()
    for copy in made:
        copy.wait()


def shards(
    groups, heads,
    hidden_in, ssm_state, conv_x_state, conv_bc_state, token_ids, ref_logits,
    in_z, in_x, in_bc, in_dt, out_t, lm_head,
    conv_wx, conv_bx, conv_wbc, conv_bbc, dt_bias, a_log, skip_gain, norm_in, norm_gain, final_gain,
):
    seqs, model = hidden_in.shape
    depth, inner = in_z.shape
    local_heads = a_log.shape[0]
    state_size = ssm_state.shape[3]
    chips = groups // 2
    half, rows = chips * seqs, groups * seqs
    wide = depth + (-depth % 128 or 128)
    vocab = lm_head.shape[0]
    width = vocab // PARTS
    cols = 2 * inner + in_bc.shape[1] + 128
    dt_rows = -(-local_heads // 16) * 16
    bf16, f32 = jnp.bfloat16, jnp.float32
    vmem, hbm = pl.BlockSpec(memory_space=pltpu.VMEM), pl.BlockSpec(memory_space=pltpu.HBM)
    smem, any_spec = pl.BlockSpec(memory_space=pltpu.SMEM), pl.BlockSpec(memory_space=pl.ANY)
    scratch = pltpu.VMEM
    dma = pltpu.SemaphoreType.DMA
    units = 3 * PIECES + 1
    slots = max(chips, 5)
    gathered = [(groups * depth, in_z.shape[1]), (groups * depth, in_x.shape[1]),
                (groups, depth, in_bc.shape[1]), (groups * depth, out_t.shape[1])]
    made = pl.pallas_call(
        functools.partial(step_kernel, groups, heads, local_heads),
        out_shape=[pltpu.VMEM(ssm_state.shape, f32)] + [pltpu.VMEM(shape, bf16) for shape in gathered]
        + [pltpu.VMEM((groups, dt_rows, wide), bf16), pltpu.VMEM((seqs, 128), f32)],
        in_specs=[vmem] * 3 + [smem] + [vmem] * 12 + [hbm] * 6,
        out_specs=[vmem] * 7,
        scratch_shapes=[
            scratch(in_bc.shape, bf16), scratch((8, 128), f32), scratch((depth, vocab), bf16),
            scratch((groups, seqs, wide), bf16), scratch((groups, seqs, wide), bf16),
            scratch((2, half, cols), bf16), scratch((half, cols), bf16),
            scratch((chips, seqs, cols), bf16), scratch((chips, seqs, cols), bf16),
            scratch((128, wide), bf16),
            scratch((seqs, 1, inner), f32), scratch((seqs, 1, state_size), f32), scratch((seqs, 1, state_size), f32),
            scratch((seqs, 1, 128), f32), scratch((seqs, 1, inner), f32),
            scratch((groups, seqs, inner), bf16),
            scratch((heads, rows, wide), bf16),
            scratch((PARTS, 2, half, width), bf16), scratch((PARTS, half, width), bf16),
            scratch((PARTS, chips, seqs, width), bf16), scratch((PARTS, chips, seqs, width), bf16),
            scratch((2, half, 128), bf16), scratch((half, 128), bf16),
            scratch((chips, seqs, 128), bf16), scratch((chips, seqs, 128), bf16),
            scratch((heads, seqs, 128), f32),
            dma((7,)), dma((units, slots)), dma((units, slots)), dma((units, slots)), dma((units, slots)),
            dma((groups,)), dma((groups,)), dma((2, chips)), dma((2, chips)), dma, dma,
            dma((chips,)), dma((chips,)), dma((2, chips)), dma((2, chips)),
            dma((heads,)), dma((heads,)), dma((PARTS + 1,)), dma((PARTS + 1,)),
            dma((PARTS + 1, chips)), dma((PARTS + 1, chips)), dma((heads,)), dma((heads,)),
            dma((heads,)), dma((heads,)), dma((heads,)), dma((heads,)),
        ],
        compiler_params=pltpu.CompilerParams(
            collective_id=0, has_side_effects=True, vmem_limit_bytes=32 * 1024 * 1024),
        name="step",
    )(
        hidden_in, conv_x_state.transpose(1, 0, 2), conv_bc_state.transpose(1, 0, 2), token_ids, ref_logits, in_dt.T,
        dt_bias, a_log, skip_gain, conv_wx, conv_bx, conv_wbc, conv_bbc, norm_in, norm_gain, final_gain,
        ssm_state, in_z, in_x, in_bc, out_t, lm_head.T,
    )
    new_state, *rolls, dt_all, result = made
    count = len(rolls) + 1
    published = pl.pallas_call(
        functools.partial(publish_kernel, count),
        out_shape=[jax.ShapeDtypeStruct(ssm_state.shape, f32)] + [jax.ShapeDtypeStruct(v, bf16) for v in gathered]
        + [jax.ShapeDtypeStruct((local_heads, model), bf16)] + [jax.ShapeDtypeStruct((1, seqs), f32)] * 2,
        in_specs=[any_spec] * count + [vmem] * 2,
        out_specs=[any_spec] * (count + 3),
        scratch_shapes=[dma((count + 1, 4)), scratch((local_heads, model), bf16)] + [scratch((1, seqs), f32)] * 2,
        compiler_params=pltpu.CompilerParams(vmem_limit_bytes=1 * 1024 * 1024),
        name="publish",
    )(new_state, *rolls, dt_all, result)
    new_state, roll_z, roll_x, roll_bc, roll_out, roll_dt, divergence, logprob = published
    roll_bc = roll_bc.reshape(model, -1)
    return new_state, divergence[0], logprob[0], roll_z, roll_x, roll_bc, roll_dt.T, roll_out


def solution(mesh):
    return jax.shard_map(
        functools.partial(shards, mesh.shape["group"], mesh.shape["head"]),
        mesh=mesh,
        in_specs=(
            P("group", None),
            P("group", "head", None, None),
            P("group", None, "head"),
            P("group", None, None),
            P("group"),
            P("group", "head"),
            P("group", "head"),
            P("group", "head"),
            P("group", None),
            P("group", "head"),
            P("group", "head"),
            P("head", "group"),
            P(None, "head"),
            P("head"),
            P(),
            P(),
            P("head"),
            P("head"),
            P("head"),
            P(),
            P("head"),
            P(),
        ),
        out_specs=(
            P("group", "head", None, None),
            P("group"),
            P("group"),
            P(None, "head"),
            P(None, "head"),
            P(),
            P(None, "head"),
            P(None, "head"),
        ),
        check_vma=False,
    )
```

```python
import functools

import jax
import jax.numpy as jnp
from jax import lax
from jax.experimental import pallas as pl
from jax.experimental.pallas import tpu as pltpu
from jax.sharding import PartitionSpec as P

P_SIZE = 64
EPSILON = 1e-05
AHEAD = 3
PIECES = 5
PARTS = 5
MESH = pl.DeviceIdType.MESH


def flip(value, mask):
    bit = 1
    while bit <= mask:
        if mask & bit:
            value = value + bit * (1 - 2 * ((value // bit) % 2))
        bit *= 2
    return value


def greet(groups, heads):
    barrier = pltpu.get_barrier_semaphore()
    group, head = lax.axis_index("group"), lax.axis_index("head")
    for j in range(1, groups):
        pl.semaphore_signal(barrier, inc=1, device_id={"group": (group + j) % groups}, device_id_type=MESH)
    for j in range(1, heads):
        pl.semaphore_signal(barrier, inc=1, device_id={"head": (head + j) % heads}, device_id_type=MESH)
    pl.semaphore_wait(barrier, groups - 1 + heads - 1)


class Links:
    def __init__(self):
        self.pending = []

    def send(self, src, dst, device, ssem, rsem):
        made = pltpu.make_async_remote_copy(
            src_ref=src, dst_ref=dst, send_sem=ssem, recv_sem=rsem, device_id=device, device_id_type=MESH)
        made.start()
        self.pending.append(made)
        return made

    def drain(self):
        for made in self.pending:
            made.wait_send()


class Bulk:
    def __init__(self, links, chips, units, send, recv, psend, precv):
        self.links, self.chips, self.units = links, chips, units
        self.sems, self.pair_sems = (send, recv), (psend, precv)
        group = lax.axis_index("group")
        self.chip, self.core = group // 2, group % 2
        self.relay = chips == 4
        self.peers = (1, 2) if self.relay else range(1, chips)
        self.far, self.near = {}, {}
        self.next, self.fed = 0, 0
        self.feed(2)

    def feed(self, ahead):
        while self.fed < min(self.next + ahead, len(self.units)):
            self.own(self.fed)
            self.fed += 1

    def rows(self, k, chip, part=None):
        src, dst, first, count = self.units[k]
        if part is not None:
            count = count // 2
            first = first + part * count
        group = chip * 2 + self.core
        if len(dst.shape) == 3:
            return dst.at[group, pl.ds(first, count)]
        return dst.at[pl.ds(pl.multiple_of(group * src.shape[0] + first, 16), count)]

    def across(self, k, m, src, dst, slot):
        send, recv = self.sems
        device = {"group": flip(self.chip, m) * 2 + self.core}
        self.far[k, slot] = self.links.send(src, dst, device, send.at[k, slot], recv.at[k, slot])

    def hand(self, k, src, dst, slot):
        send, recv = self.pair_sems
        device = {"group": self.chip * 2 + 1 - self.core}
        self.near.setdefault(k, []).append(self.links.send(src, dst, device, send.at[k, slot], recv.at[k, slot]))

    def own(self, k):
        src, _, first, count = self.units[k]
        src, dst = src.at[pl.ds(first, count)], self.rows(k, self.chip)
        for m in self.peers:
            self.across(k, m, src, dst, m)
        self.hand(k, src, dst, 0)

    def step(self, ahead):
        k = self.next
        self.next += 1
        for m in self.peers:
            self.far[k, m].wait_recv()
            for by, part, slot in self.relays(k):
                if by == m:
                    view = self.rows(k, flip(self.chip, m), part)
                    self.across(k, 3 - m, view, view, slot)
            view = self.rows(k, flip(self.chip, m))
            self.hand(k, view, view, m)
        self.feed(ahead)
        if k:
            self.last(k - 1)

    def relays(self, k):
        if not self.relay:
            return []
        return [(1, 0, 3), (2, 1, 4)] if self.units[k][3] % 32 == 0 else [(1, None, 3)]

    def last(self, k):
        for _, part, slot in self.relays(k):
            self.far[k, slot].wait_recv()
            view = self.rows(k, flip(self.chip, 3), part)
            self.hand(k, view, view, slot)

    def pump(self, count, ahead=AHEAD):
        for _ in range(count):
            if self.next < len(self.units):
                self.step(ahead)

    def finish(self):
        self.pump(len(self.units))
        self.last(len(self.units) - 1)
        for k in range(len(self.units)):
            self.arrive(k)

    def arrive(self, k):
        for made in self.near.pop(k, []):
            made.wait_recv()


class Scatter:
    def __init__(self, links, chips, chip, core, blocks, middle, ends, send_sems, recv_sems):
        self.blocks, self.middle, self.ends = blocks, middle, ends
        self.two_phases = chips == 4
        columns = blocks.shape[2]
        cut = -(-columns // 256) * 128
        self.parts = slice(0, cut), slice(cut, columns)

        def send(src, dst, m, slot):
            device = {"group": flip(chip, m) * 2 + core}
            return links.send(src, dst, device, send_sems(slot), recv_sems(slot))

        self.send = send
        if self.two_phases:
            left, right = (pl.ds(part.start, part.stop - part.start) for part in self.parts)
            self.sent = [
                send(blocks.at[pl.ds(1, 2), :, left], middle.at[pl.ds(0, 2), :, left], 1, 0),
                send(blocks.at[pl.ds(2, 2), :, right], middle.at[pl.ds(0, 2), :, right], 2, 1)]
        else:
            self.sent = [send(blocks.at[m], middle.at[m - 1], m, m) for m in range(1, chips)]

    def turn(self):
        if not self.two_phases:
            return
        for n, (block, arrived, m) in enumerate(((3, 1, 2), (1, 0, 1))):
            self.sent[n].wait_recv()
            part = self.parts[n]
            passed = self.blocks[block, :, part].astype(jnp.float32) + self.middle[arrived, :, part].astype(jnp.float32)
            self.blocks[block, :, part] = passed.astype(jnp.bfloat16)
            columns = pl.ds(part.start, part.stop - part.start)
            self.sent.append(self.send(self.blocks.at[block, :, columns], self.ends.at[:, columns], m, 2 + n))

    def total(self):
        for made in self.sent[2:] if self.two_phases else self.sent:
            made.wait_recv()
        f32 = jnp.float32
        if not self.two_phases:
            return self.blocks[0].astype(f32) + jnp.sum(self.middle[...].astype(f32), axis=0)
        return jnp.concatenate(
            [self.blocks[0, :, part].astype(f32) + self.middle[n, :, part].astype(f32)
             + self.ends[:, part].astype(f32) for n, part in enumerate(self.parts)], axis=1)


def halves(column, lanes, first, split):
    high = column.astype(jnp.bfloat16).astype(jnp.float32)
    return jnp.where(lanes < split, high, column - high)


def rms_scale(mean_square):
    return lax.rsqrt(mean_square + EPSILON)


def silu(values):
    return values * jax.nn.sigmoid(values)


def window(values, first, width):
    wide = width + (-width % 128 or 128)
    span = wide + 128
    start = min(first // 128 * 128, values.shape[1] - span)
    return pltpu.roll(values[:, start:start + span], (start - first) % span, 1)[:, :wide]


def own_window(values, group, groups, width):
    chosen = window(values, 0, width)
    for p in range(1, groups):
        chosen = jnp.where(group == p, window(values, p * width, width), chosen)
    return chosen


def step_kernel(
    groups, heads, local_heads,
    hid_ref, cx_ref, cbc_ref, token_ref, refl_ref, dt_ref, bias_ref, rate_ref, skip_ref,
    wx_ref, bx_ref, wbc_ref, bbc_ref, norm_in_ref, ngain_ref, fgain_ref,
    state_hbm, z_hbm, x_hbm, bc_hbm, out_hbm, lm_hbm,
    new_ref, z_all, x_all, bc_all, out_all, dt_all, result_ref,
    bc_own, small_ref, lm_ref, hsend, hall, ppairs, ppair_in, psum, psum_mid, psum_end, dt_pad, inflow_ref, b_ref, c_ref, decay_ref, y_ref,
    gall, mix, pairs, pair_in, sums, sums_mid, sums_end, square, square_in, squares_out, squares_in, stat,
    load, bsend, brecv, bpsend, bprecv, hsem, hrsem, dsem, drsem, qsem, qrsem, rsem, rrsem, gsem, grsem,
    msend, mrecv, psend, precv, ssend, srecv, tsend, trecv, zsem, zrsem, ysem, yrsem,
):
    f32, bf16 = jnp.float32, jnp.bfloat16
    chips = groups // 2
    group, head = lax.axis_index("group"), lax.axis_index("head")
    chip, core = group // 2, group % 2
    seqs, model = hid_ref.shape
    depth, inner = z_hbm.shape
    wide = hall.shape[2]
    half, rows = chips * seqs, groups * seqs
    vocab = lm_ref.shape[1]
    parts, width = pairs.shape[0], pairs.shape[3]
    state_size = b_ref.shape[2]
    links = Links()
    send = links.send
    order = (0, 1, 3, 2) if chips == 4 else tuple(range(chips))
    chip_rows = [pl.ds(pl.multiple_of(flip(chip, r) * seqs, 16), seqs) for r in order]
    slot_of = lambda g: (g % 2) * chips + g // 2
    mine = slot_of(group)
    other = {"group": chip * 2 + 1 - core}

    loads = []

    def fetch(src, dst):
        made = pltpu.make_async_copy(src, dst, load.at[len(loads)])
        made.start()
        loads.append(made)
        return made

    own_rows = pl.ds(pl.multiple_of(group * depth, 16), depth)
    have = [fetch(src, dst) for src, dst in (
        (z_hbm, z_all.at[own_rows]), (x_hbm, x_all.at[own_rows]),
        (bc_hbm, bc_own), (out_hbm, out_all.at[own_rows]))]
    split = depth % (16 * heads) == 0
    share_rows = depth // heads if split else depth
    share_at = pl.multiple_of(head * share_rows, 16) if split else 0
    have_share = fetch(bc_hbm.at[pl.ds(share_at, share_rows)], bc_all.at[group, pl.ds(share_at, share_rows)])
    have_state = fetch(state_hbm, new_ref)
    have_lm = fetch(lm_hbm, lm_ref)

    hid = hid_ref[...].astype(f32)
    mean_square = jnp.mean(hid * hid, axis=-1, keepdims=True)
    lanes = lax.broadcasted_iota(jnp.int32, (seqs, wide), 1)
    middle = (depth + wide) // 2
    square_halves = halves(mean_square, lanes, depth, middle)
    for p in range(groups):
        hsend[p] = jnp.where(lanes < depth, window(hid, p * depth, depth), square_halves).astype(bf16)
    dt_pad[...] = jnp.zeros_like(dt_pad)
    dt_pad[0:local_heads, 0:depth] = dt_ref[...]
    small_ref[...] = jnp.zeros_like(small_ref)
    for n, ref in enumerate((bias_ref, rate_ref, skip_ref)):
        small_ref[n:n + 1, 0:local_heads] = ref[...][None, :]

    greet(groups, heads)
    first, dts = [], []
    for j in range(1, groups):
        peer = (group + j) % groups
        first.append(send(hsend.at[peer], hall.at[mine], {"group": peer}, hsem.at[j], hrsem.at[j]))
    dt_rows = dt_all.shape[1]
    for m in range(1, chips):
        dts.append(send(dt_pad.at[pl.ds(0, dt_rows)], dt_all.at[group], {"group": flip(chip, m) * 2 + core},
                        dsem.at[0, m], drsem.at[0, m]))
    dts.append(send(dt_pad.at[pl.ds(0, dt_rows)], dt_all.at[group], other, dsem.at[1, 0], drsem.at[1, 0]))
    piece = depth // PIECES
    units = [(bc_hbm, bc_all, share_at, share_rows)]
    for src, dst in ((z_hbm, z_all), (x_hbm, x_all), (out_hbm, out_all)):
        units += [(src, dst, n * piece, piece) for n in range(PIECES)]
    bulk = Bulk(links, chips, units, bsend, brecv, bpsend, bprecv)

    hall[mine] = hsend[group]
    dt_all[group] = dt_pad[0:dt_rows]
    norm_gain = own_window(norm_in_ref[...][None, :], group, groups, depth)
    final_gain = own_window(fgain_ref[...][None, :], group, groups, depth)
    for made in have[:3]:
        made.wait()
    for made in first:
        made.wait_recv()
    hidden = hall[...].reshape(rows, wide).astype(f32)
    mean_square = hidden[:, depth:depth + 1] + hidden[:, middle:middle + 1]
    normed = (hidden * rms_scale(mean_square) * norm_gain).astype(bf16)[:, :depth]
    at = 0
    for weights in (z_all[own_rows, :], x_all[own_rows, :], bc_own[...]):
        cols = weights.shape[1]
        made = jnp.dot(normed, weights, preferred_element_type=f32).astype(bf16)
        ppairs[0, :, at:at + cols], ppairs[1, :, at:at + cols] = made[:half], made[half:]
        at += cols
    made = lax.dot_general(
        normed, dt_pad[:, 0:depth], (((1,), (1,)), ((), ())), preferred_element_type=f32).astype(bf16)
    ppairs[0, :, at:at + 128], ppairs[1, :, at:at + 128] = made[:half], made[half:]
    handed = send(ppairs.at[1 - core], ppair_in, other, qsem, qrsem)
    for m in range(1, chips):
        dts[m - 1].wait_recv()
        view = dt_all.at[flip(chip, m) * 2 + core]
        dts.append(send(view, view, other, dsem.at[1, m], drsem.at[1, m]))
    handed.wait_recv()
    for n, these in enumerate(chip_rows):
        psum[n] = (ppairs[core, these, :].astype(f32) + ppair_in[these, :].astype(f32)).astype(bf16)
    branches = Scatter(
        links, chips, chip, core, psum, psum_mid, psum_end, lambda k: rsem.at[k], lambda k: rrsem.at[k])
    bulk.pump(1)
    branches.turn()
    bulk.pump(1)
    branch = branches.total().astype(bf16).astype(f32)

    def conv(history, newest, taps, offset):
        total = newest * taps[history.shape[0]:, :]
        for n in range(history.shape[0]):
            total += history[n].astype(f32) * taps[n:n + 1, :]
        return silu(total + offset[None, :])

    gate = branch[:, :inner]
    x_conv = conv(cx_ref[...], branch[:, inner:2 * inner], wx_ref[...], bx_ref[...])
    bc_conv = conv(cbc_ref[...], branch[:, 2 * inner:2 * inner + 2 * state_size], wbc_ref[...], bbc_ref[...])
    raw = branch[:, 2 * inner + 2 * state_size:] + small_ref[0:1, :]
    step = jnp.maximum(raw, 0.0) + jnp.log1p(jnp.exp(-jnp.abs(raw)))
    decay = jnp.exp(-step * jnp.exp(small_ref[1:2, :]))
    place = lax.broadcasted_iota(jnp.int32, (128, inner), 0) * P_SIZE
    lane = lax.broadcasted_iota(jnp.int32, (128, inner), 1)
    chosen = jnp.where((lane >= place) & (lane < place + P_SIZE), 1.0, 0.0)
    by_head = jnp.concatenate([step, jnp.broadcast_to(small_ref[2:3, :], (8, 128))], axis=0)
    by_column = jnp.dot(by_head, chosen, preferred_element_type=f32, precision=lax.Precision.HIGHEST)
    inflow = by_column[:seqs] * x_conv
    skip = by_column[seqs:seqs + 1] * x_conv
    for s in range(seqs):
        inflow_ref[s] = inflow[s:s + 1]
        b_ref[s] = bc_conv[s:s + 1, :state_size]
        c_ref[s] = bc_conv[s:s + 1, state_size:]
        decay_ref[s] = decay[s:s + 1]
    have_state.wait()

    def pair(row):
        high = row.astype(bf16).astype(f32)
        return high, row - high

    def one(s):
        high, low = pair(inflow_ref[s])
        b_high, b_low = pair(b_ref[s])
        place = lax.broadcasted_iota(jnp.int32, (16, inner), 0)
        left = jnp.where(place < 2, high, jnp.where(place < 4, low, 0.0)).astype(bf16)
        place = lax.broadcasted_iota(jnp.int32, (16, state_size), 0)
        right = jnp.where(place % 2 == 0, b_high, b_low).astype(bf16)
        flow = lax.dot_general(left, right, (((0,), (0,)), ((), ())), preferred_element_type=f32)
        decays = decay_ref[s]
        for h in range(local_heads):
            new_ref[s, h] = decays[:, h:h + 1] * new_ref[s, h] + flow[h * P_SIZE:(h + 1) * P_SIZE]
        new = new_ref[s].reshape(inner, state_size).astype(bf16)
        c = jnp.broadcast_to(c_ref[s], (16, state_size)).astype(bf16)
        y = lax.dot_general(c, new, (((1,), (1,)), ((), ())), preferred_element_type=f32)
        y_ref[s] = y[0:1]

    bulk.pump(1)
    passed, crossed = [], []
    have_share.wait()
    if split:
        bulk.arrive(0)
        for j in range(1, heads):
            view = bc_all.at[pl.ds(core * chips, chips), pl.ds(share_at, share_rows)]
            crossed.append(send(view, view, {"head": (head + j) % heads}, zsem.at[j], zrsem.at[j]))
    for n in range(4):
        pl.loop(n * seqs // 4, (n + 1) * seqs // 4)(one)
        bulk.pump(1, 3 if n < 3 else 2)
    for j, made in enumerate(crossed, 1):
        made.wait_recv()
        first_row = pl.multiple_of((head - j + heads) % heads * share_rows, 16)
        view = bc_all.at[pl.ds(core * chips, chips), pl.ds(first_row, share_rows)]
        passed.append(send(view, view, other, ysem.at[j], yrsem.at[j]))

    ssm_out = jnp.concatenate([y_ref[s] for s in range(seqs)], axis=0) + skip
    gall[mine] = (ssm_out * silu(gate)).astype(bf16)
    sent = [send(gall.at[mine], gall.at[mine], {"group": flip(chip, m) * 2 + core}, gsem.at[0, m], grsem.at[0, m])
            for m in range(1, chips)]
    near = [send(gall.at[mine], gall.at[mine], other, gsem.at[1, 0], grsem.at[1, 0])]
    bulk.pump(1)
    for m in range(1, chips):
        sent[m - 1].wait_recv()
        view = gall.at[core * chips + flip(chip, m)]
        near.append(send(view, view, other, gsem.at[1, m], grsem.at[1, m]))
    for made in near:
        made.wait_recv()
    have[3].wait()

    gated = gall[...].reshape(rows, inner).astype(f32)
    squares = jnp.sum(gated * gated, axis=-1, keepdims=True)
    scaled = (gated * ngain_ref[...][None, :]).astype(bf16)
    out_rows = out_all[own_rows, :]
    out_rows = jnp.concatenate([out_rows, jnp.zeros((wide - depth, inner), bf16)], axis=0)
    partial = lax.dot_general(scaled, out_rows, (((1,), (1,)), ((), ())), preferred_element_type=f32)
    lanes = lax.broadcasted_iota(jnp.int32, (rows, wide), 1)
    mix[0] = jnp.where(lanes < depth, partial, halves(squares, lanes, depth, middle)).astype(bf16)
    mixes = [
        send(mix.at[0], mix.at[j], {"head": (head + j) % heads}, msend.at[j], mrecv.at[j])
        for j in range(1, heads)
    ]
    bulk.pump(1, 4)
    have_lm.wait()
    for made in mixes:
        made.wait_recv()
    total = jnp.sum(mix[...].astype(f32), axis=0)
    square_total = total[:, depth:depth + 1] + total[:, middle:middle + 1]
    stream = hidden + total * rms_scale(square_total / (inner * heads))
    stream = jnp.where(lanes < depth, stream, 0.0)
    final_squares = jnp.sum(stream * stream, axis=-1, keepdims=True)
    final = (stream * final_gain).astype(bf16)[:, :depth]
    tail_lanes = lax.broadcasted_iota(jnp.int32, (rows, 128), 1)
    packed = halves(jnp.broadcast_to(final_squares, (rows, 128)), tail_lanes, 0, 64).astype(bf16)
    square[0], square[1] = packed[:half], packed[half:]
    pair_sends = [send(square.at[1 - core], square_in, other, psend.at[parts], precv.at[parts])]
    last, scatters = [], []

    def join(t):
        pair_sends[t + 1].wait_recv()
        for n, these in enumerate(chip_rows):
            sums[t, n] = (pairs[t, core, these, :].astype(f32) + pair_in[t, these, :].astype(f32)).astype(bf16)
        scatters.append(Scatter(
            links, chips, chip, core, sums.at[t], sums_mid.at[t], sums_end.at[t],
            lambda k: ssend.at[t, k], lambda k: srecv.at[t, k]))

    for t in range(parts):
        block = jnp.dot(
            final, lm_ref[:, t * width:(t + 1) * width], preferred_element_type=f32).astype(bf16)
        pairs[t, 0], pairs[t, 1] = block[:half], block[half:]
        pair_sends.append(send(pairs.at[t, 1 - core], pair_in.at[t], other, psend.at[t], precv.at[t]))
        if t == 0:
            pair_sends[0].wait_recv()
            rest = square[core].astype(f32) + square_in[...].astype(f32)
            rest = rest[:, 0:1] + rest[:, 64:65]
            split = halves(rest, lax.broadcasted_iota(jnp.int32, (half, 128), 1), 0, 64)
            squares_out[...] = split.astype(bf16).reshape(chips, seqs, 128)
            for m in range(1, chips):
                peer = flip(chip, m)
                last.append(send(
                    squares_out.at[peer], squares_in.at[m], {"group": peer * 2 + core},
                    ssend.at[parts, m], srecv.at[parts, m]))
            squares_in[0] = squares_out[chip]
        else:
            join(t - 1)
    join(parts - 1)
    bulk.pump(1)
    for scatter in scatters:
        scatter.turn()
    bulk.pump(1)
    for made in last:
        made.wait_recv()
    bulk.pump(1)

    square_sum = jnp.sum(squares_in[...].astype(f32), axis=0)
    mean_square = (square_sum[:, 0:1] + square_sum[:, 64:65]) / model
    logits = jnp.concatenate([scatter.total() for scatter in scatters], axis=1)
    logits = logits * rms_scale(mean_square)
    reference = refl_ref[...].astype(f32)
    row = lax.broadcasted_iota(jnp.int32, (seqs, 128), 0)
    tokens = jnp.zeros((seqs, 128), jnp.int32)
    for s in range(seqs):
        tokens = jnp.where(row == s, token_ref[s], tokens)
    columns = lax.broadcasted_iota(jnp.int32, (seqs, vocab), 1) + head * vocab
    picked = jnp.sum(jnp.where(columns == tokens[:, 0:1], logits, 0.0), axis=-1, keepdims=True)
    top = jnp.max(logits, axis=-1, keepdims=True)
    ref_top = jnp.max(reference, axis=-1, keepdims=True)
    weights = jnp.exp(reference - ref_top)
    values = (
        top,
        jnp.sum(jnp.exp(logits - top), axis=-1, keepdims=True),
        ref_top,
        jnp.sum(weights, axis=-1, keepdims=True),
        jnp.sum(weights * (reference - logits), axis=-1, keepdims=True),
        picked,
    )
    slot = lax.broadcasted_iota(jnp.int32, (seqs, 128), 1)
    mine_values = jnp.zeros((seqs, 128), f32)
    for n, value in enumerate(values):
        mine_values = jnp.where(slot == n, value, mine_values)
    stat[0] = mine_values
    stats = [
        send(stat.at[0], stat.at[j], {"head": (head + j) % heads}, tsend.at[j], trecv.at[j])
        for j in range(1, heads)
    ]
    for made in stats:
        made.wait_recv()
    every = stat[...]
    pick = lambda n: every[:, :, n:n + 1]
    top = jnp.max(pick(0), axis=0)
    ref_top = jnp.max(pick(2), axis=0)
    factor = jnp.exp(pick(0) - top[None])
    ref_factor = jnp.exp(pick(2) - ref_top[None])
    roll_sum = jnp.sum(pick(1) * factor, axis=0)
    ref_sum = jnp.sum(pick(3) * ref_factor, axis=0)
    cross = jnp.sum(pick(4) * ref_factor, axis=0)
    picked = jnp.sum(pick(5), axis=0)
    lse_roll = top + jnp.log(roll_sum)
    lse_ref = ref_top + jnp.log(ref_sum)
    result_ref[...] = jnp.where(slot == 0, cross / ref_sum - lse_ref + lse_roll, picked - lse_roll)

    bulk.finish()
    for made in passed:
        made.wait_recv()
    for made in dts[chips - 1:]:
        made.wait_recv()
    links.drain()


def publish_kernel(count, *refs):
    ins, dt_ref, result_ref = refs[:count], refs[count], refs[count + 1]
    outs, smalls, (sems, *held) = refs[count + 2:2 * count + 2], refs[2 * count + 2:2 * count + 5], refs[2 * count + 5:]
    dt_out, div_out, prob_out = held
    made = []
    for n, (src, dst) in enumerate(zip(ins, outs)):
        size = src.shape[0] // 4
        for p in range(4):
            rows = pl.ds(p * size, size)
            made.append(pltpu.make_async_copy(src.at[rows], dst.at[rows], sems.at[n, p]))
            made[-1].start()
    local_heads, model = dt_out.shape
    groups = dt_ref.shape[0]
    depth = model // groups
    dt_out[...] = jnp.concatenate(
        [dt_ref[g].astype(jnp.float32)[:, :depth] for g in range(groups)], axis=1
    )[:local_heads].astype(dt_out.dtype)
    seqs = div_out.shape[1]
    result = result_ref[...]
    same = lax.broadcasted_iota(jnp.int32, (seqs, seqs), 0) == lax.broadcasted_iota(jnp.int32, (seqs, seqs), 1)
    for n, ref in enumerate((div_out, prob_out)):
        ref[...] = jnp.sum(jnp.where(same, result[:, n:n + 1], 0.0), axis=0, keepdims=True)
    for n, (src, dst) in enumerate(zip(held, smalls)):
        made.append(pltpu.make_async_copy(src, dst, sems.at[count, n]))
        made[-1].start()
    for copy in made:
        copy.wait()


def shards(
    groups, heads,
    hidden_in, ssm_state, conv_x_state, conv_bc_state, token_ids, ref_logits,
    in_z, in_x, in_bc, in_dt, out_t, lm_head,
    conv_wx, conv_bx, conv_wbc, conv_bbc, dt_bias, a_log, skip_gain, norm_in, norm_gain, final_gain,
):
    seqs, model = hidden_in.shape
    depth, inner = in_z.shape
    local_heads = a_log.shape[0]
    state_size = ssm_state.shape[3]
    chips = groups // 2
    half, rows = chips * seqs, groups * seqs
    wide = depth + (-depth % 128 or 128)
    vocab = lm_head.shape[0]
    width = vocab // PARTS
    cols = 2 * inner + in_bc.shape[1] + 128
    dt_rows = -(-local_heads // 16) * 16
    bf16, f32 = jnp.bfloat16, jnp.float32
    vmem, hbm = pl.BlockSpec(memory_space=pltpu.VMEM), pl.BlockSpec(memory_space=pltpu.HBM)
    smem, any_spec = pl.BlockSpec(memory_space=pltpu.SMEM), pl.BlockSpec(memory_space=pl.ANY)
    scratch = pltpu.VMEM
    dma = pltpu.SemaphoreType.DMA
    units = 3 * PIECES + 1
    slots = max(chips, 5)
    steps = 2 if chips == 4 else chips - 1
    gathered = [(groups * depth, in_z.shape[1]), (groups * depth, in_x.shape[1]),
                (groups, depth, in_bc.shape[1]), (groups * depth, out_t.shape[1])]
    made = pl.pallas_call(
        functools.partial(step_kernel, groups, heads, local_heads),
        out_shape=[pltpu.VMEM(ssm_state.shape, f32)] + [pltpu.VMEM(shape, bf16) for shape in gathered]
        + [pltpu.VMEM((groups, dt_rows, wide), bf16), pltpu.VMEM((seqs, 128), f32)],
        in_specs=[vmem] * 3 + [smem] + [vmem] * 12 + [hbm] * 6,
        out_specs=[vmem] * 7,
        scratch_shapes=[
            scratch(in_bc.shape, bf16), scratch((8, 128), f32), scratch((depth, vocab), bf16),
            scratch((groups, seqs, wide), bf16), scratch((groups, seqs, wide), bf16),
            scratch((2, half, cols), bf16), scratch((half, cols), bf16),
            scratch((chips, seqs, cols), bf16), scratch((steps, seqs, cols), bf16), scratch((seqs, cols), bf16),
            scratch((128, wide), bf16),
            scratch((seqs, 1, inner), f32), scratch((seqs, 1, state_size), f32), scratch((seqs, 1, state_size), f32),
            scratch((seqs, 1, 128), f32), scratch((seqs, 1, inner), f32),
            scratch((groups, seqs, inner), bf16),
            scratch((heads, rows, wide), bf16),
            scratch((PARTS, 2, half, width), bf16), scratch((PARTS, half, width), bf16),
            scratch((PARTS, chips, seqs, width), bf16),
            scratch((PARTS, steps, seqs, width), bf16), scratch((PARTS, seqs, width), bf16),
            scratch((2, half, 128), bf16), scratch((half, 128), bf16),
            scratch((chips, seqs, 128), bf16), scratch((chips, seqs, 128), bf16),
            scratch((heads, seqs, 128), f32),
            dma((7,)), dma((units, slots)), dma((units, slots)), dma((units, slots)), dma((units, slots)),
            dma((groups,)), dma((groups,)), dma((2, chips)), dma((2, chips)), dma, dma,
            dma((chips,)), dma((chips,)), dma((2, chips)), dma((2, chips)),
            dma((heads,)), dma((heads,)), dma((PARTS + 1,)), dma((PARTS + 1,)),
            dma((PARTS + 1, chips)), dma((PARTS + 1, chips)), dma((heads,)), dma((heads,)),
            dma((heads,)), dma((heads,)), dma((heads,)), dma((heads,)),
        ],
        compiler_params=pltpu.CompilerParams(
            collective_id=0, has_side_effects=True, vmem_limit_bytes=32 * 1024 * 1024),
        name="step",
    )(
        hidden_in, conv_x_state.transpose(1, 0, 2), conv_bc_state.transpose(1, 0, 2), token_ids, ref_logits, in_dt.T,
        dt_bias, a_log, skip_gain, conv_wx, conv_bx, conv_wbc, conv_bbc, norm_in, norm_gain, final_gain,
        ssm_state, in_z, in_x, in_bc, out_t, lm_head.T,
    )
    new_state, *rolls, dt_all, result = made
    count = len(rolls) + 1
    published = pl.pallas_call(
        functools.partial(publish_kernel, count),
        out_shape=[jax.ShapeDtypeStruct(ssm_state.shape, f32)] + [jax.ShapeDtypeStruct(v, bf16) for v in gathered]
        + [jax.ShapeDtypeStruct((local_heads, model), bf16)] + [jax.ShapeDtypeStruct((1, seqs), f32)] * 2,
        in_specs=[any_spec] * count + [vmem] * 2,
        out_specs=[any_spec] * (count + 3),
        scratch_shapes=[dma((count + 1, 4)), scratch((local_heads, model), bf16)] + [scratch((1, seqs), f32)] * 2,
        compiler_params=pltpu.CompilerParams(vmem_limit_bytes=1 * 1024 * 1024),
        name="publish",
    )(new_state, *rolls, dt_all, result)
    new_state, roll_z, roll_x, roll_bc, roll_out, roll_dt, divergence, logprob = published
    roll_bc = roll_bc.reshape(model, -1)
    return new_state, divergence[0], logprob[0], roll_z, roll_x, roll_bc, roll_dt.T, roll_out


def solution(mesh):
    return jax.shard_map(
        functools.partial(shards, mesh.shape["group"], mesh.shape["head"]),
        mesh=mesh,
        in_specs=(
            P("group", None),
            P("group", "head", None, None),
            P("group", None, "head"),
            P("group", None, None),
            P("group"),
            P("group", "head"),
            P("group", "head"),
            P("group", "head"),
            P("group", None),
            P("group", "head"),
            P("group", "head"),
            P("head", "group"),
            P(None, "head"),
            P("head"),
            P(),
            P(),
            P("head"),
            P("head"),
            P("head"),
            P(),
            P("head"),
            P(),
        ),
        out_specs=(
            P("group", "head", None, None),
            P("group"),
            P("group"),
            P(None, "head"),
            P(None, "head"),
            P(),
            P(None, "head"),
            P(None, "head"),
        ),
        check_vma=False,
    )
```
